128 devices in a mesh: fsdp: 16 (over y, x_hi, core), tp: 8 (over z, x_lo).
Axes of the slice: x: 4 (x_hi: 2, x_lo: 2; x = x_hi * 2 + x_lo), y: 4, z: 4, core: 2. Of those that a mesh axis runs over, the one named last changes fastest.
Arguments:
- w_gate: float32 [3072, 8192], P('fsdp', 'tp'), may hold values from -0.15625 to 0.15625
- first_gate: float32 [3072, 8192], P('fsdp', 'tp'), may hold values from -0.109375 to 0.109375
- second_gate: float32 [3072, 8192], P('fsdp', 'tp'), may hold values from -0.109375 to 0.109375
- w_up: float32 [3072, 8192], P('fsdp', 'tp'), may hold values from -0.15625 to 0.15625
- first_up: float32 [3072, 8192], P('fsdp', 'tp'), may hold values from -0.109375 to 0.109375
- second_up: float32 [3072, 8192], P('fsdp', 'tp'), may hold values from -0.109375 to 0.109375
- norm_train: float32 [3072], P(('fsdp', 'tp')), may hold values from 0.25 to 1.75
- norm_step: float32 [3072], P(('fsdp', 'tp')), may hold values from -0.3 to 0.3
Outputs:
- serving_gate: bfloat16 [3072, 8192], P(None, 'tp')
- serving_up: bfloat16 [3072, 8192], P(None, 'tp')
- scale_gate: float32 [8192], P('tp')
- scale_up: float32 [8192], P('tp')
- serve_norm: bfloat16 [3072], replicated
- whole_gate: float32 [3072, 8192], P('fsdp', 'tp')
- whole_up: float32 [3072, 8192], P('fsdp', 'tp')
The draws below stay inside these ranges and needn't reach their ends.
All inputs are finite; a program needn't handle non-finite values. Where the reference program divides by a largest or mean magnitude, that divisor is 1e-20 or more.
Results may differ from the reference program's by a relative error of at most 0.001.
Values may be sent and summed in bfloat16 or wider, within the bound.
A program may use at most 128 MiB of HBM per device.

```python
import jax
import jax.numpy as jnp

D_MODEL = 3072
D_INNER = 8192


def spiked(entries, rng, source, target, shards_of, factor):
    owner, partner = [(jnp.arange(entries.shape[axis_at]) // (entries.shape[axis_at] // shards_of)).reshape([-1 if axis == axis_at else 1 for axis in range(entries.ndim)]) for axis_at in (source, target)]
    chosen = jax.random.permutation(rng, shards_of)[partner]
    strong = (owner == chosen) | (owner == (partner + shards_of // 2) % shards_of)
    return jnp.where(strong, factor * entries, entries)


def levels(own_key, extent, cuts, least, top_value):
    def one(position, shards_of):
        draws = jax.random.uniform(jax.random.fold_in(jax.random.fold_in(own_key, 6), position), (shards_of,), jnp.float32, least / len(cuts), top_value / len(cuts))
        return jnp.repeat(jnp.exp(draws), extent[position] // shards_of).reshape((-1,) + (1,) * (len(extent) - position - 1))

    loudness = one(*cuts[0])
    for cut in cuts[1:]:
        loudness = loudness * one(*cut)
    return loudness


def noise(rng, dims, width, bound, split=(), held_as=jnp.bfloat16):
    values = width * jax.random.normal(rng, dims, jnp.float32)
    if split:
        values = values * levels(rng, dims, split, -0.22, 0.18)
    return jnp.clip(values, -bound, bound).astype(held_as)


def bell_draw_with(key, shape, deviation, reach, pieces, heavy, dtype=jnp.bfloat16):
    result = deviation * jax.random.normal(key, shape, jnp.float32)
    if pieces:
        result = result * levels(key, shape, pieces, -0.22, 0.18)
    return jnp.clip(spiked(result, jax.random.fold_in(key, 3), *heavy), -reach, reach).astype(dtype)


def setup_inputs(seed: int = 0) -> dict:
    arg_keys = jax.random.split(jax.random.key(seed), 9)
    return {
        "w_gate": bell_draw_with(arg_keys[0], (D_MODEL, D_INNER), D_MODEL ** -0.5, 0.15625, ((0, 16), (1, 8)), (0, 1, 16, 2.0), jnp.float32),
        "first_gate": noise(arg_keys[1], (D_MODEL, D_INNER), D_MODEL ** -0.5, 0.109375, ((0, 16), (1, 8)), jnp.float32),
        "second_gate": noise(arg_keys[2], (D_MODEL, D_INNER), D_MODEL ** -0.5, 0.109375, ((0, 16), (1, 8)), jnp.float32),
        "w_up": bell_draw_with(arg_keys[3], (D_MODEL, D_INNER), D_MODEL ** -0.5, 0.15625, ((0, 16), (1, 8)), (0, 1, 16, 2.0), jnp.float32),
        "first_up": noise(arg_keys[4], (D_MODEL, D_INNER), D_MODEL ** -0.5, 0.109375, ((0, 16), (1, 8)), jnp.float32),
        "second_up": noise(arg_keys[5], (D_MODEL, D_INNER), D_MODEL ** -0.5, 0.109375, ((0, 16), (1, 8)), jnp.float32),
        "norm_train": jnp.clip(1.0 + 0.15 * jax.random.normal(arg_keys[6], (D_MODEL,), jnp.float32), 0.25, 1.75),
        "norm_step": jnp.clip(jax.random.uniform(arg_keys[7], (D_MODEL,), jnp.float32, -0.3, 0.3) * levels(arg_keys[7], (D_MODEL,), ((0, 128),), -0.4, 0.0), -0.3, 0.3),
    }


learn_rate = 0.25
hold_rate = 0.9


def reference(w_gate, first_gate, second_gate, w_up, first_up, second_up, norm_train, norm_step):
    hold_gate = hold_rate * first_gate + second_gate
    whole_gate = w_gate - learn_rate * hold_gate
    hold_up = hold_rate * first_up + second_up
    whole_up = w_up - learn_rate * hold_up
    scale_gate = jnp.sum(jnp.abs(whole_gate), axis=0) / D_MODEL
    serving_gate = (whole_gate / scale_gate).astype(jnp.bfloat16)
    scale_up = jnp.sum(jnp.abs(whole_up), axis=0) / D_MODEL
    serving_up = (whole_up / scale_up).astype(jnp.bfloat16)
    serve_norm = (norm_train + norm_step).astype(jnp.bfloat16)
    return serving_gate, serving_up, scale_gate, scale_up, serve_norm, whole_gate, whole_up
```

```python
import functools

import jax
import jax.numpy as jnp
from jax import lax
from jax.experimental import pallas as pl
from jax.experimental.pallas import tpu as pltpu
from jax.sharding import PartitionSpec as P

MESH = pl.DeviceIdType.MESH
LEARN_RATE = 0.25
HOLD_RATE = 0.9

UNITS = ((0, 64, 1, False), (96, 64, -1, False), (64, 32, 1, True), (160, 32, -1, True))
A, B, C, D, E, F, G = range(7)


def kernel(
    d_model, wg, fg, sg, wu, fu, su, nt, ns,
    serve_g, serve_u, scale_g, scale_u, norm_out, whole_g, whole_u,
    a1, a2, b1, b2, n0, n1, part, own_norm, near, far, norm,
    in_sem, tree_send, tree_recv, part_send, part_recv, norm_send, norm_recv, d2d_send, d2d_recv,
):
    f, t = lax.axis_index("fsdp"), lax.axis_index("tp")
    y, p, c = f // 4, (f // 2) % 2, f % 2

    def at(dy, dp, dc):
        return ((y + dy + 4) % 4) * 4 + ((p + dp) % 2) * 2 + (c + dc) % 2

    peers = [at(dy, dp, dc) for dy in (2, 1, 3, 0) for dp in (1, 0) for dc in (1, 0) if (dy, dp, dc) != (0, 0, 0)]
    peers_tp = [(t + k) % 8 for k in range(1, 8)]

    barrier = pltpu.get_barrier_semaphore()
    for q in peers:
        pl.semaphore_signal(barrier, inc=1, device_id=(q, t), device_id_type=MESH)
    for q in peers_tp:
        pl.semaphore_signal(barrier, inc=1, device_id=(f, q), device_id_type=MESH)

    serve, scale = (serve_g, serve_u), (scale_g, scale_u)
    pairs = ((wg, whole_g), (fg, a1), (sg, a2), (wu, whole_u), (fu, b1), (su, b2), (nt, n0), (ns, n1))
    loads = [pltpu.make_async_copy(src, dst, in_sem.at[i]) for i, (src, dst) in enumerate(pairs)]
    for load in loads:
        load.start()

    def remote(src, dst, send, recv, q):
        return pltpu.make_async_remote_copy(
            src_ref=src, dst_ref=dst, send_sem=send, recv_sem=recv, device_id=(q, t), device_id_type=MESH
        )

    def update(g, w, m1, m2):
        whole = w[...] - LEARN_RATE * (HOLD_RATE * m1[...] + m2[...])
        w[...] = whole
        part[g, f] = jnp.sum(jnp.abs(whole), axis=0, keepdims=True)

    def share(g):
        for q in peers:
            remote(part.at[g, f], part.at[g, f], part_send.at[g], part_recv.at[g], q).start()

    def narrow(g, w):
        pltpu.make_async_copy(part.at[g, pl.ds(0, 15)], part.at[g, pl.ds(0, 15)], part_recv.at[g]).wait()
        mean = jnp.sum(part[g], axis=0) / d_model
        scale[g][...] = mean
        serve[g][f] = (w[...] * (1.0 / mean)).astype(jnp.bfloat16)

    def rows(g, u, block):
        return serve[g].at[block, pl.ds(UNITS[u][0], UNITS[u][1])]

    late = []

    def send(g, u, kind, block, q):
        cp = remote(rows(g, u, block), rows(g, u, block), tree_send.at[g, u, kind], tree_recv.at[g, u, kind], q)
        cp.start()
        late.append(cp.wait_send)

    def arrived(g, u, kind, block):
        remote(rows(g, u, block), rows(g, u, block), tree_send.at[g, u, kind], tree_recv.at[g, u, kind], f).wait_recv()

    given = []

    def swap(g, dy, dp):
        block, k = at(dy, dp, 0), dy * 2 + dp
        return remote(serve[g].at[block], serve[g].at[block], d2d_send.at[g, k], d2d_recv.at[g, k], at(0, 0, 1))

    def give(g, dy, dp):
        cp = swap(g, dy, dp)
        cp.start()
        late.append(cp.wait_send)
        given.append((g, dy, dp))

    def take():
        g, dy, dp = given.pop(0)
        block, k = at(dy, dp, 1), dy * 2 + dp
        remote(serve[g].at[block], serve[g].at[block], d2d_send.at[g, k], d2d_recv.at[g, k], f).wait_recv()

    def own(g):
        for u, (_, _, s, _) in enumerate(UNITS):
            send(g, u, A, f, at(s, 0, 0))
            send(g, u, C, f, at(0, 1, 0))
            send(g, u, B, f, at(-s, 0, 0))

    for load in loads[:3]:
        load.wait()
    update(0, whole_g, a1, a2)
    pl.semaphore_wait(barrier, len(peers) + len(peers_tp))
    share(0)
    for load in loads[3:6]:
        load.wait()
    update(1, whole_u, b1, b2)
    share(1)
    narrow(0, whole_g)
    own(0)
    narrow(1, whole_u)
    own(1)

    for load in loads[6:]:
        load.wait()
    own_norm[...] = jnp.zeros_like(own_norm)
    own_norm[0:1, 0:24] = (n0[...] + n1[...]).astype(jnp.bfloat16).astype(jnp.float32)
    first = 24 * t + 64 * (f % 2)
    rolled = pltpu.roll(jnp.broadcast_to(own_norm[0:1, :], (8, 128)), first % 128, 1)
    place = 128 * lax.broadcasted_iota(jnp.int32, (8, 128), 0) + lax.broadcasted_iota(jnp.int32, (8, 128), 1) - first
    near[t] = jnp.where((place >= 0) & (place < 24), rolled, 0.0)
    for q in peers_tp:
        pltpu.make_async_remote_copy(
            src_ref=near.at[t], dst_ref=near.at[t], send_sem=norm_send.at[0], recv_sem=norm_recv.at[0],
            device_id=(f, q), device_id_type=MESH,
        ).start()

    for g in (0, 1):
        give(g, 0, 0)

    for g in (0, 1):
        for u, (_, _, s, three) in enumerate(UNITS):
            arrived(g, u, A, at(-s, 0, 0))
            send(g, u, D, at(-s, 0, 0), at(s, 0, 0))
            send(g, u, E, at(-s, 0, 0), at(0, 1, 0))
            arrived(g, u, C, at(0, 1, 0))
            if not three:
                send(g, u, F, at(0, 1, 0), at(-s, 0, 0))
        give(g, 0, 1)
        take()
        if g == 0:
            pltpu.make_async_copy(near.at[pl.ds(0, 7)], near.at[pl.ds(0, 7)], norm_recv.at[0]).wait()
            far[f] = jnp.sum(near[...], axis=0)
            for q in peers:
                remote(far.at[f], far.at[f], norm_send.at[1], norm_recv.at[1], q).start()
    for g in (0, 1):
        for u, (_, _, s, three) in enumerate(UNITS):
            arrived(g, u, B, at(s, 0, 0))
            if three:
                send(g, u, F, at(s, 0, 0), at(0, 1, 0))
        give(g, 1, 0)
        give(g, 3, 0)
        take()
    for g in (0, 1):
        for u, (_, _, s, _) in enumerate(UNITS):
            arrived(g, u, E, at(-s, 1, 0))
            send(g, u, G, at(-s, 1, 0), at(s, 0, 0))
        take()
    for g in (0, 1):
        for u in range(len(UNITS)):
            arrived(g, u, D, at(2, 0, 0))
        give(g, 2, 0)
        take()

    pltpu.make_async_copy(far.at[pl.ds(0, 15)], far.at[pl.ds(0, 15)], norm_recv.at[1]).wait()
    norm[...] = jnp.zeros_like(norm)
    for i in range(16):
        r = 3 * i // 2
        norm[r : r + 2, :] = norm[r : r + 2, :] + far[i, 0:2, :]
    norm_out[...] = norm[0:24, :].astype(jnp.bfloat16)

    for g in (0, 1):
        for u, (_, _, s, _) in enumerate(UNITS):
            arrived(g, u, F, at(s, 1, 0))
        give(g, 1, 1)
        give(g, 3, 1)
        take()
        take()
    for g in (0, 1):
        for u in range(len(UNITS)):
            arrived(g, u, G, at(2, 1, 0))
        give(g, 2, 1)
        take()
    while given:
        take()

    for g in (0, 1):
        pltpu.make_async_copy(part.at[g, pl.ds(0, 15)], part.at[g, pl.ds(0, 15)], part_send.at[g]).wait()
    pltpu.make_async_copy(near.at[pl.ds(0, 7)], near.at[pl.ds(0, 7)], norm_send.at[0]).wait()
    pltpu.make_async_copy(far.at[pl.ds(0, 15)], far.at[pl.ds(0, 15)], norm_send.at[1]).wait()
    for wait in late:
        wait()


def keep(*refs):
    n = len(refs) // 2
    copies = [pltpu.make_async_copy(refs[i], refs[n + i], refs[-1].at[i]) for i in range(n)]
    for cp in copies:
        cp.start()
    for cp in copies:
        cp.wait()


def per_device(d_model, *args):
    rows, cols = args[0].shape
    f32, bf16 = jnp.float32, jnp.bfloat16
    any_space, vmem = pl.BlockSpec(memory_space=pl.ANY), pl.BlockSpec(memory_space=pltpu.VMEM)
    dma = pltpu.SemaphoreType.DMA
    shapes = (
        ((16, rows, cols), bf16),
        ((16, rows, cols), bf16),
        ((1, cols), f32),
        ((1, cols), f32),
        ((24, 128), bf16),
        ((rows, cols), f32),
        ((rows, cols), f32),
    )
    args = (*args[:6], *(a.reshape(1, -1) for a in args[6:]))
    args = [pltpu.with_memory_space_constraint(a, pltpu.HBM) for a in args]
    held = pl.pallas_call(
        functools.partial(kernel, d_model),
        name="step",
        out_shape=tuple(pltpu.VMEM(*shape) for shape in shapes),
        in_specs=[any_space] * 8,
        out_specs=[vmem] * 7,
        scratch_shapes=[
            *[pltpu.VMEM((rows, cols), f32)] * 4,
            *[pltpu.VMEM((1, 24), f32)] * 2,
            pltpu.VMEM((2, 16, 1, cols), f32),
            pltpu.VMEM((8, 128), f32),
            pltpu.VMEM((8, 8, 128), f32),
            pltpu.VMEM((16, 8, 128), f32),
            pltpu.VMEM((32, 128), f32),
            dma((8,)), dma((2, 4, 7)), dma((2, 4, 7)), dma((2,)), dma((2,)), dma((2,)), dma((2,)), dma((2, 8)), dma((2, 8)),
        ],
        compiler_params=pltpu.CompilerParams(collective_id=0, has_side_effects=True, vmem_limit_bytes=16 * 2**20),
    )(*args)
    outs = pl.pallas_call(
        keep,
        name="keep",
        out_shape=tuple(jax.ShapeDtypeStruct(*shape) for shape in shapes),
        in_specs=[vmem] * 7,
        out_specs=[any_space] * 7,
        scratch_shapes=[dma((7,))],
        compiler_params=pltpu.CompilerParams(has_side_effects=True, vmem_limit_bytes=2**20),
    )(*[pltpu.with_memory_space_constraint(a, pltpu.VMEM) for a in held])
    serving_gate, serving_up, scale_gate, scale_up, norm, whole_gate, whole_up = outs
    return (
        serving_gate.reshape(16 * rows, cols),
        serving_up.reshape(16 * rows, cols),
        scale_gate.reshape(cols),
        scale_up.reshape(cols),
        norm.reshape(-1),
        whole_gate,
        whole_up,
    )


def solution(mesh):
    split = P("fsdp", "tp")
    return jax.shard_map(
        functools.partial(per_device, 3072),
        mesh=mesh,
        in_specs=(split,) * 6 + (P(("fsdp", "tp")),) * 2,
        out_specs=(P(None, "tp"), P(None, "tp"), P("tp"), P("tp"), P(), split, split),
        check_vma=False,
    )
```

```python
import functools

import jax
import jax.numpy as jnp
from jax import lax
from jax.experimental import pallas as pl
from jax.experimental.pallas import tpu as pltpu
from jax.sharding import PartitionSpec as P

MESH = pl.DeviceIdType.MESH
LEARN_RATE = 0.25
HOLD_RATE = 0.9

UNITS = ((0, 64, 1, False), (96, 64, -1, False), (64, 32, 1, True), (160, 32, -1, True))
KINDS = "ABCDEFG"


def semaphore_of(kind, u):
    three = UNITS[u][3]
    k = KINDS.index(kind)
    if kind in "AE" or (kind == "B" and three) or (kind == "C" and not three):
        return (k, u)
    return (k, "late" if kind in "FG" and three else "all")


SEMAPHORES = sorted({semaphore_of(kind, u) for kind in KINDS for u in range(4)}, key=str)
TOGETHER = {key: tuple((KINDS[key[0]], u) for u in range(4) if semaphore_of(KINDS[key[0]], u) == key) for key in SEMAPHORES}


def kernel(
    d_model, wg, fg, sg, wu, fu, su, nt, ns,
    serve_g, serve_u, scale_g, scale_u, norm_out, whole_g, whole_u,
    a1, a2, b1, b2, n0, n1, part, own_norm, near, far, norm,
    in_sem, sent, tree_recv, part_recv, norm_send, norm_recv, d2d_recv, here,
):
    f, t = lax.axis_index("fsdp"), lax.axis_index("tp")
    y, p, c = f // 4, (f // 2) % 2, f % 2

    def at(dy, dp, dc):
        return ((y + dy + 4) % 4) * 4 + ((p + dp) % 2) * 2 + (c + dc) % 2

    peers = [at(dy, dp, dc) for dy in (2, 1, 3, 0) for dp in (1, 0) for dc in (1, 0) if (dy, dp, dc) != (0, 0, 0)]

    barrier = pltpu.get_barrier_semaphore()
    for q in peers:
        pl.semaphore_signal(barrier, inc=1, device_id=(q, t), device_id_type=MESH)
    for q in range(1, 8):

        @pl.when(t < q)
        def _(q=q):
            pl.semaphore_signal(barrier, inc=1, device_id=(f, q), device_id_type=MESH)

    serve, scale = (serve_g, serve_u), (scale_g, scale_u)
    pairs = ((wg, whole_g), (fg, a1), (sg, a2), (wu, whole_u), (fu, b1), (su, b2), (nt, n0), (ns, n1))
    loads = [pltpu.make_async_copy(src, dst, in_sem.at[i]) for i, (src, dst) in enumerate(pairs)]
    for load in loads:
        load.start()

    def remote(src, dst, send, recv, q):
        return pltpu.make_async_remote_copy(
            src_ref=src, dst_ref=dst, send_sem=send, recv_sem=recv, device_id=(q, t), device_id_type=MESH
        )

    def update(w, m1, m2, g):
        whole = w[...] - LEARN_RATE * (HOLD_RATE * m1[...] + m2[...])
        w[...] = whole
        part[g, f] = jnp.sum(jnp.abs(whole), axis=0, keepdims=True)

    def share(g):
        for q in peers:
            remote(part.at[g, f], part.at[g, f], sent.at[2], part_recv.at[g], q).start()

    def narrow(g, w):
        pltpu.make_async_copy(part.at[g, pl.ds(0, 15)], part.at[g, pl.ds(0, 15)], part_recv.at[g]).wait()
        mean = jnp.sum(part[g], axis=0) / d_model
        scale[g][...] = mean
        serve[g][f] = (w[...] * (1.0 / mean)).astype(jnp.bfloat16)

    def rows(g, u, block):
        return serve[g].at[block, pl.ds(UNITS[u][0], UNITS[u][1])]

    def send(g, u, kind, block, q):
        k = SEMAPHORES.index(semaphore_of(kind, u))
        remote(rows(g, u, block), rows(g, u, block), sent.at[g], tree_recv.at[g, k], q).start()

    def arrived(g, kind, u):
        key = semaphore_of(kind, u)
        total = sum(UNITS[v][1] for _, v in TOGETHER[key])
        ref = serve[g].at[0, pl.ds(0, total)]
        pltpu.make_async_copy(ref, ref, tree_recv.at[g, SEMAPHORES.index(key)]).wait()

    def give(g, dy, dp, units=None):
        block, k = at(dy, dp, 0), dy * 2 + dp
        for ref in [serve[g].at[block]] if units is None else [rows(g, u, block) for u in units]:
            remote(ref, ref, sent.at[g], d2d_recv.at[g, k], at(0, 0, 1)).start()

    def own(g):
        for u, (_, _, s, _) in enumerate(UNITS):
            send(g, u, "A", f, at(s, 0, 0))
            send(g, u, "C", f, at(0, 1, 0))
            send(g, u, "B", f, at(-s, 0, 0))

    for load in loads[:3]:
        load.wait()
    update(whole_g, a1, a2, 0)
    pl.semaphore_wait(barrier, len(peers) + t)
    share(0)
    for load in loads[3:6]:
        load.wait()
    update(whole_u, b1, b2, 1)
    share(1)
    for q in range(7):

        @pl.when(t > q)
        def _(q=q):
            pl.semaphore_signal(here, inc=1, device_id=(f, q), device_id_type=MESH)

    for load in loads[6:]:
        load.wait()
    own_norm[...] = jnp.zeros_like(own_norm)
    own_norm[0:1, 0:24] = (n0[...] + n1[...]).astype(jnp.bfloat16).astype(jnp.float32)
    first = 24 * t + 64 * (f % 2)
    rolled = pltpu.roll(jnp.broadcast_to(own_norm[0:1, :], (8, 128)), first % 128, 1)
    place = 128 * lax.broadcasted_iota(jnp.int32, (8, 128), 0) + lax.broadcasted_iota(jnp.int32, (8, 128), 1) - first
    near[t] = jnp.where((place >= 0) & (place < 24), rolled, 0.0)[0:2]

    narrow(0, whole_g)
    own(0)
    narrow(1, whole_u)
    own(1)
    for g in (0, 1):
        give(g, 0, 0)

    @pl.when(t < 7)
    def _():
        pl.semaphore_wait(here, 7 - t)

    for k in range(1, 8):
        pltpu.make_async_remote_copy(
            src_ref=near.at[t], dst_ref=near.at[t], send_sem=norm_send.at[0], recv_sem=norm_recv.at[0],
            device_id=(f, (t + k) % 8), device_id_type=MESH,
        ).start()

    for g in (0, 1):
        for u, (_, _, s, three) in enumerate(UNITS):
            arrived(g, "A", u)
            send(g, u, "D", at(-s, 0, 0), at(s, 0, 0))
            send(g, u, "E", at(-s, 0, 0), at(0, 1, 0))
            if not three:
                arrived(g, "C", u)
                send(g, u, "F", at(0, 1, 0), at(-s, 0, 0))
        arrived(g, "C", 2)
        give(g, 0, 1)
    for g in (0, 1):
        for u in (2, 3):
            s = UNITS[u][2]
            arrived(g, "B", u)
            send(g, u, "F", at(s, 0, 0), at(0, 1, 0))
        arrived(g, "B", 0)
        give(g, 1, 0)
        give(g, 3, 0)

    pltpu.make_async_copy(near.at[pl.ds(0, 7)], near.at[pl.ds(0, 7)], norm_recv.at[0]).wait()
    far[f] = jnp.sum(near[...], axis=0)
    for q in peers:
        remote(far.at[f], far.at[f], norm_send.at[1], norm_recv.at[1], q).start()

    for g in (0, 1):
        for u, (_, _, s, _) in enumerate(UNITS):
            arrived(g, "E", u)
            send(g, u, "G", at(-s, 1, 0), at(s, 0, 0))
    for g in (0, 1):
        arrived(g, "D", 0)
        give(g, 2, 0)

    pltpu.make_async_copy(far.at[pl.ds(0, 15)], far.at[pl.ds(0, 15)], norm_recv.at[1]).wait()
    norm[...] = jnp.zeros_like(norm)
    for i in range(16):
        r = 3 * i // 2
        norm[r : r + 2, :] = norm[r : r + 2, :] + far[i]
    norm_out[...] = norm[0:24, :].astype(jnp.bfloat16)

    for g in (0, 1):
        arrived(g, "F", 0)
        give(g, 1, 1, (0, 1, 3))
        give(g, 3, 1, (0, 1, 2))
    for g in (0, 1):
        arrived(g, "G", 0)
        give(g, 2, 1, (0, 1))
        arrived(g, "F", 2)
        give(g, 1, 1, (2,))
        give(g, 3, 1, (3,))
        arrived(g, "G", 2)
        give(g, 2, 1, (2, 3))

    for g in (0, 1):
        for k in range(8):
            pltpu.make_async_copy(serve[g].at[0], serve[g].at[0], d2d_recv.at[g, k]).wait()
    for g in (0, 1):
        pltpu.make_async_copy(serve[g].at[pl.ds(0, 15)], serve[g].at[pl.ds(0, 15)], sent.at[g]).wait()
    pltpu.make_async_copy(part.at[:, pl.ds(0, 15)], part.at[:, pl.ds(0, 15)], sent.at[2]).wait()
    pltpu.make_async_copy(near.at[pl.ds(0, 7)], near.at[pl.ds(0, 7)], norm_send.at[0]).wait()
    pltpu.make_async_copy(far.at[pl.ds(0, 15)], far.at[pl.ds(0, 15)], norm_send.at[1]).wait()


def keep(*refs):
    n = len(refs) // 2
    copies = [pltpu.make_async_copy(refs[i], refs[n + i], refs[-1].at[i]) for i in range(n)]
    for cp in copies:
        cp.start()
    for cp in copies:
        cp.wait()


def per_device(d_model, *args):
    rows, cols = args[0].shape
    f32, bf16 = jnp.float32, jnp.bfloat16
    any_space, vmem = pl.BlockSpec(memory_space=pl.ANY), pl.BlockSpec(memory_space=pltpu.VMEM)
    dma = pltpu.SemaphoreType.DMA
    shapes = (
        ((16, rows, cols), bf16),
        ((16, rows, cols), bf16),
        ((1, cols), f32),
        ((1, cols), f32),
        ((24, 128), bf16),
        ((rows, cols), f32),
        ((rows, cols), f32),
    )
    args = (*args[:6], *(a.reshape(1, -1) for a in args[6:]))
    args = [pltpu.with_memory_space_constraint(a, pltpu.HBM) for a in args]
    held = pl.pallas_call(
        functools.partial(kernel, d_model),
        name="step",
        out_shape=tuple(pltpu.VMEM(*shape) for shape in shapes),
        in_specs=[any_space] * 8,
        out_specs=[vmem] * 7,
        scratch_shapes=[
            *[pltpu.VMEM((rows, cols), f32)] * 4,
            *[pltpu.VMEM((1, 24), f32)] * 2,
            pltpu.VMEM((2, 16, 1, cols), f32),
            pltpu.VMEM((8, 128), f32),
            pltpu.VMEM((8, 2, 128), f32),
            pltpu.VMEM((16, 2, 128), f32),
            pltpu.VMEM((32, 128), f32),
            dma((8,)), dma((3,)), dma((2, len(SEMAPHORES))), dma((2,)), dma((2,)), dma((2,)), dma((2, 8)), pltpu.SemaphoreType.REGULAR,
        ],
        compiler_params=pltpu.CompilerParams(collective_id=0, has_side_effects=True, vmem_limit_bytes=16 * 2**20),
    )(*args)
    outs = pl.pallas_call(
        keep,
        name="keep",
        out_shape=tuple(jax.ShapeDtypeStruct(*shape) for shape in shapes),
        in_specs=[vmem] * 7,
        out_specs=[any_space] * 7,
        scratch_shapes=[dma((7,))],
        compiler_params=pltpu.CompilerParams(has_side_effects=True, vmem_limit_bytes=2**20),
    )(*[pltpu.with_memory_space_constraint(a, pltpu.VMEM) for a in held])
    serving_gate, serving_up, scale_gate, scale_up, norm, whole_gate, whole_up = outs
    return (
        serving_gate.reshape(16 * rows, cols),
        serving_up.reshape(16 * rows, cols),
        scale_gate.reshape(cols),
        scale_up.reshape(cols),
        norm.reshape(-1),
        whole_gate,
        whole_up,
    )


def solution(mesh):
    split = P("fsdp", "tp")
    return jax.shard_map(
        functools.partial(per_device, 3072),
        mesh=mesh,
        in_specs=(split,) * 6 + (P(("fsdp", "tp")),) * 2,
        out_specs=(P(None, "tp"), P(None, "tp"), P("tp"), P("tp"), P(), split, split),
        check_vma=False,
    )
```

```python
import functools

import jax
import jax.numpy as jnp
from jax import lax
from jax.experimental import pallas as pl
from jax.experimental.pallas import tpu as pltpu
from jax.sharding import PartitionSpec as P

MESH = pl.DeviceIdType.MESH
LEARN_RATE = 0.25
HOLD_RATE = 0.9

UNITS = (
    ((0, 72, 1, False), (96, 72, -1, False), (72, 24, 1, True), (168, 24, -1, True)),
    ((0, 64, 1, False), (96, 64, -1, False), (64, 32, 1, True), (160, 32, -1, True)),
)
KINDS = "ABCDEFG"


def semaphore_of(kind, u):
    three = UNITS[0][u][3]
    k = KINDS.index(kind)
    if kind in "AE" or (kind == "B" and three) or (kind == "C" and not three):
        return (k, u)
    return (k, "late" if kind in "FG" and three else "all")


SEMAPHORES = sorted({semaphore_of(kind, u) for kind in KINDS for u in range(4)}, key=str)
TOGETHER = {key: tuple((KINDS[key[0]], u) for u in range(4) if semaphore_of(KINDS[key[0]], u) == key) for key in SEMAPHORES}


def kernel(
    d_model, wg, fg, sg, wu, fu, su, nt, ns,
    serve_g, serve_u, scale_g, scale_u, norm_out, whole_g, whole_u,
    a1, a2, b1, b2, n0, n1, part, own_norm, near, far, norm,
    in_sem, sent, tree_recv, part_recv, norm_send, norm_recv, d2d_recv, here,
):
    f, t = lax.axis_index("fsdp"), lax.axis_index("tp")
    y, p, c = f // 4, (f // 2) % 2, f % 2

    def at(dy, dp, dc):
        return ((y + dy + 4) % 4) * 4 + ((p + dp) % 2) * 2 + (c + dc) % 2

    peers = [at(dy, dp, dc) for dy in (2, 1, 3, 0) for dp in (1, 0) for dc in (1, 0) if (dy, dp, dc) != (0, 0, 0)]

    barrier = pltpu.get_barrier_semaphore()
    for q in peers:
        pl.semaphore_signal(barrier, inc=1, device_id=(q, t), device_id_type=MESH)
    for q in range(1, 8):

        @pl.when(t < q)
        def _(q=q):
            pl.semaphore_signal(barrier, inc=1, device_id=(f, q), device_id_type=MESH)

    serve, scale = (serve_g, serve_u), (scale_g, scale_u)
    pairs = ((wg, whole_g), (fg, a1), (sg, a2), (wu, whole_u), (fu, b1), (su, b2), (nt, n0), (ns, n1))
    loads = [pltpu.make_async_copy(src, dst, in_sem.at[i]) for i, (src, dst) in enumerate(pairs)]
    for load in loads:
        load.start()

    def remote(src, dst, send, recv, q):
        return pltpu.make_async_remote_copy(
            src_ref=src, dst_ref=dst, send_sem=send, recv_sem=recv, device_id=(q, t), device_id_type=MESH
        )

    def update(w, m1, m2, g):
        whole = w[...] - LEARN_RATE * (HOLD_RATE * m1[...] + m2[...])
        w[...] = whole
        part[g, f] = jnp.sum(jnp.abs(whole), axis=0, keepdims=True)

    def share(g):
        for q in peers:
            remote(part.at[g, f], part.at[g, f], sent.at[2], part_recv.at[g], q).start()

    def narrow(g, w):
        pltpu.make_async_copy(part.at[g, pl.ds(0, 15)], part.at[g, pl.ds(0, 15)], part_recv.at[g]).wait()
        mean = jnp.sum(part[g], axis=0) / d_model
        scale[g][...] = mean
        serve[g][f] = (w[...] * (1.0 / mean)).astype(jnp.bfloat16)

    def rows(g, u, block):
        return serve[g].at[block, pl.ds(UNITS[g][u][0], UNITS[g][u][1])]

    def send(g, u, kind, block, q):
        k = SEMAPHORES.index(semaphore_of(kind, u))
        remote(rows(g, u, block), rows(g, u, block), sent.at[g], tree_recv.at[g, k], q).start()

    def arrived(g, kind, u):
        key = semaphore_of(kind, u)
        total = sum(UNITS[g][v][1] for _, v in TOGETHER[key])
        ref = serve[g].at[0, pl.ds(0, total)]
        pltpu.make_async_copy(ref, ref, tree_recv.at[g, SEMAPHORES.index(key)]).wait()

    def give(g, dy, dp, units=None):
        block, k = at(dy, dp, 0), dy * 2 + dp
        for ref in [serve[g].at[block]] if units is None else [rows(g, u, block) for u in units]:
            remote(ref, ref, sent.at[g], d2d_recv.at[g, k], at(0, 0, 1)).start()

    def own(g):
        for u, (_, _, s, _) in enumerate(UNITS[g]):
            send(g, u, "A", f, at(s, 0, 0))
            send(g, u, "C", f, at(0, 1, 0))
            send(g, u, "B", f, at(-s, 0, 0))

    for load in loads[:3]:
        load.wait()
    update(whole_g, a1, a2, 0)
    pl.semaphore_wait(barrier, len(peers) + t)
    share(0)
    for load in loads[3:6]:
        load.wait()
    update(whole_u, b1, b2, 1)
    share(1)
    for q in range(7):

        @pl.when(t > q)
        def _(q=q):
            pl.semaphore_signal(here, inc=1, device_id=(f, q), device_id_type=MESH)

    for load in loads[6:]:
        load.wait()
    own_norm[...] = jnp.zeros_like(own_norm)
    own_norm[0:1, 0:24] = (n0[...] + n1[...]).astype(jnp.bfloat16).astype(jnp.float32)
    first = 24 * t + 64 * (f % 2)
    rolled = pltpu.roll(jnp.broadcast_to(own_norm[0:1, :], (8, 128)), first % 128, 1)
    place = 128 * lax.broadcasted_iota(jnp.int32, (8, 128), 0) + lax.broadcasted_iota(jnp.int32, (8, 128), 1) - first
    near[t] = jnp.where((place >= 0) & (place < 24), rolled, 0.0)[0:2]

    narrow(0, whole_g)
    own(0)
    @pl.when(t < 7)
    def _():
        pl.semaphore_wait(here, 7 - t)

    for k in range(1, 8):
        pltpu.make_async_remote_copy(
            src_ref=near.at[t], dst_ref=near.at[t], send_sem=norm_send.at[0], recv_sem=norm_recv.at[0],
            device_id=(f, (t + k) % 8), device_id_type=MESH,
        ).start()
    narrow(1, whole_u)
    own(1)
    for g in (0, 1):
        give(g, 0, 0)

    for g in (0, 1):
        for u, (_, _, s, three) in enumerate(UNITS[g]):
            arrived(g, "A", u)
            send(g, u, "D", at(-s, 0, 0), at(s, 0, 0))
            send(g, u, "E", at(-s, 0, 0), at(0, 1, 0))
            if not three:
                arrived(g, "C", u)
                send(g, u, "F", at(0, 1, 0), at(-s, 0, 0))
        arrived(g, "C", 2)
        give(g, 0, 1)
        if g == 0:
            pltpu.make_async_copy(near.at[pl.ds(0, 7)], near.at[pl.ds(0, 7)], norm_recv.at[0]).wait()
            far[f] = jnp.sum(near[...], axis=0)
            for q in peers:
                remote(far.at[f], far.at[f], norm_send.at[1], norm_recv.at[1], q).start()
    for g in (0, 1):
        for u in (2, 3):
            s = UNITS[g][u][2]
            arrived(g, "B", u)
            send(g, u, "F", at(s, 0, 0), at(0, 1, 0))
        arrived(g, "B", 0)
        give(g, 1, 0)
        give(g, 3, 0)

    for g in (0, 1):
        for u, (_, _, s, _) in enumerate(UNITS[g]):
            arrived(g, "E", u)
            send(g, u, "G", at(-s, 1, 0), at(s, 0, 0))
    for g in (0, 1):
        arrived(g, "D", 0)
        give(g, 2, 0)

    pltpu.make_async_copy(far.at[pl.ds(0, 15)], far.at[pl.ds(0, 15)], norm_recv.at[1]).wait()
    norm[...] = jnp.zeros_like(norm)
    for i in range(16):
        r = 3 * i // 2
        norm[r : r + 2, :] = norm[r : r + 2, :] + far[i]
    norm_out[...] = norm[0:24, :].astype(jnp.bfloat16)

    for g in (0, 1):
        arrived(g, "F", 0)
        give(g, 1, 1, (0, 1, 3))
        give(g, 3, 1, (0, 1, 2))
    for g in (0, 1):
        arrived(g, "G", 0)
        give(g, 2, 1, (0, 1))
        arrived(g, "F", 2)
        give(g, 1, 1, (2,))
        give(g, 3, 1, (3,))
        arrived(g, "G", 2)
        give(g, 2, 1, (2, 3))

    for g in (0, 1):
        for k in range(8):
            pltpu.make_async_copy(serve[g].at[0], serve[g].at[0], d2d_recv.at[g, k]).wait()
    for g in (0, 1):
        pltpu.make_async_copy(serve[g].at[pl.ds(0, 15)], serve[g].at[pl.ds(0, 15)], sent.at[g]).wait()
    pltpu.make_async_copy(part.at[:, pl.ds(0, 15)], part.at[:, pl.ds(0, 15)], sent.at[2]).wait()
    pltpu.make_async_copy(near.at[pl.ds(0, 7)], near.at[pl.ds(0, 7)], norm_send.at[0]).wait()
    pltpu.make_async_copy(far.at[pl.ds(0, 15)], far.at[pl.ds(0, 15)], norm_send.at[1]).wait()


def keep(*refs):
    n = len(refs) // 2
    copies = [pltpu.make_async_copy(refs[i], refs[n + i], refs[-1].at[i]) for i in range(n)]
    for cp in copies:
        cp.start()
    for cp in copies:
        cp.wait()


def per_device(d_model, *args):
    rows, cols = args[0].shape
    f32, bf16 = jnp.float32, jnp.bfloat16
    any_space, vmem = pl.BlockSpec(memory_space=pl.ANY), pl.BlockSpec(memory_space=pltpu.VMEM)
    dma = pltpu.SemaphoreType.DMA
    shapes = (
        ((16, rows, cols), bf16),
        ((16, rows, cols), bf16),
        ((1, cols), f32),
        ((1, cols), f32),
        ((24, 128), bf16),
        ((rows, cols), f32),
        ((rows, cols), f32),
    )
    args = (*args[:6], *(a.reshape(1, -1) for a in args[6:]))
    args = [pltpu.with_memory_space_constraint(a, pltpu.HBM) for a in args]
    held = pl.pallas_call(
        functools.partial(kernel, d_model),
        name="step",
        out_shape=tuple(pltpu.VMEM(*shape) for shape in shapes),
        in_specs=[any_space] * 8,
        out_specs=[vmem] * 7,
        scratch_shapes=[
            *[pltpu.VMEM((rows, cols), f32)] * 4,
            *[pltpu.VMEM((1, 24), f32)] * 2,
            pltpu.VMEM((2, 16, 1, cols), f32),
            pltpu.VMEM((8, 128), f32),
            pltpu.VMEM((8, 2, 128), f32),
            pltpu.VMEM((16, 2, 128), f32),
            pltpu.VMEM((32, 128), f32),
            dma((8,)), dma((3,)), dma((2, len(SEMAPHORES))), dma((2,)), dma((2,)), dma((2,)), dma((2, 8)), pltpu.SemaphoreType.REGULAR,
        ],
        compiler_params=pltpu.CompilerParams(collective_id=0, has_side_effects=True, vmem_limit_bytes=16 * 2**20),
    )(*args)
    outs = pl.pallas_call(
        keep,
        name="keep",
        out_shape=tuple(jax.ShapeDtypeStruct(*shape) for shape in shapes),
        in_specs=[vmem] * 7,
        out_specs=[any_space] * 7,
        scratch_shapes=[dma((7,))],
        compiler_params=pltpu.CompilerParams(has_side_effects=True, vmem_limit_bytes=2**20),
    )(*[pltpu.with_memory_space_constraint(a, pltpu.VMEM) for a in held])
    serving_gate, serving_up, scale_gate, scale_up, norm, whole_gate, whole_up = outs
    return (
        serving_gate.reshape(16 * rows, cols),
        serving_up.reshape(16 * rows, cols),
        scale_gate.reshape(cols),
        scale_up.reshape(cols),
        norm.reshape(-1),
        whole_gate,
        whole_up,
    )


def solution(mesh):
    split = P("fsdp", "tp")
    return jax.shard_map(
        functools.partial(per_device, 3072),
        mesh=mesh,
        in_specs=(split,) * 6 + (P(("fsdp", "tp")),) * 2,
        out_specs=(P(None, "tp"), P(None, "tp"), P("tp"), P("tp"), P(), split, split),
        check_vma=False,
    )
```

```python
import functools

import jax
import jax.numpy as jnp
from jax import lax
from jax.experimental import pallas as pl
from jax.experimental.pallas import tpu as pltpu
from jax.sharding import PartitionSpec as P

MESH = pl.DeviceIdType.MESH
LEARN_RATE = 0.25
HOLD_RATE = 0.9

UNITS = (
    ((0, 48, 1, 2), (96, 56, -1, 2), (72, 24, 1, 3), (168, 24, -1, 3), (48, 24, 1, 2), (152, 16, -1, 2)),
    ((0, 64, 1, 2), (96, 64, -1, 2), (64, 32, 1, 3), (160, 32, -1, 3)),
)
EARLY = (4, 5)
EARLY_AT = (0, 24)
EARLY_ROWS = 40
KINDS = "ABCDEFG"


def semaphore_of(g, kind, u):
    three = UNITS[g][u][3] == 3
    if kind in "AE" or (kind == "B" and three) or (kind == "C" and not three):
        return kind, u
    return kind, 9 if kind in "FG" and three else 8


SEMAPHORES, TOGETHER = [], []
for matrix in (0, 1):
    rows_of = {}
    for kind in KINDS:
        for u, unit in enumerate(UNITS[matrix]):
            if matrix == 1 or u not in EARLY or kind not in "ABC":
                key = semaphore_of(matrix, kind, u)
                rows_of[key] = rows_of.get(key, 0) + unit[1]
    SEMAPHORES.append(sorted(rows_of))
    TOGETHER.append(rows_of)


def kernel(
    d_model, wg, fg, sg, wu, fu, su, nt, ns,
    serve_g, serve_u, scale_g, scale_u, norm_out, whole_g, whole_u,
    a1, a2, b1, b2, n0, n1, direct, part, total, own_norm, near, far, image, stack, norm, early,
    in_sem, sent, tree_recv, sums_recv, norm_sent, norm_recv, d2d_recv, early_recv, here,
):
    f, t = lax.axis_index("fsdp"), lax.axis_index("tp")
    y, p, c = f // 4, (f // 2) % 2, f % 2

    def at(dy, dp, dc):
        return ((y + dy + 4) % 4) * 4 + ((p + dp) % 2) * 2 + (c + dc) % 2

    peers = [at(dy, dp, dc) for dy in (2, 1, 3, 0) for dp in (1, 0) for dc in (1, 0) if (dy, dp, dc) != (0, 0, 0)]
    row, row_peers = f % 4, [at(0, 1, 1), at(0, 1, 0), at(0, 0, 1)]
    ring_peers = [at(2, 0, 0), at(1, 0, 0), at(3, 0, 0)]
    z, side = t // 2, t % 2
    tp_peers = [(t + 2 * k) % 8 for k in range(1, 4)] + [2 * z + 1 - side]

    barrier = pltpu.get_barrier_semaphore()
    for q in peers:
        pl.semaphore_signal(barrier, inc=1, device_id=(q, t), device_id_type=MESH)
    for q in tp_peers:

        @pl.when(t < q)
        def _(q=q):
            pl.semaphore_signal(barrier, inc=1, device_id=(f, q), device_id_type=MESH)

    serve, scale = (serve_g, serve_u), (scale_g, scale_u)
    pairs = ((wg, whole_g), (fg, a1), (sg, a2), (wu, whole_u), (fu, b1), (su, b2), (nt, n0), (ns, n1))
    loads = [pltpu.make_async_copy(src, dst, in_sem.at[i]) for i, (src, dst) in enumerate(pairs)]
    for load in loads:
        load.start()

    def remote(src, dst, send, recv, q):
        return pltpu.make_async_remote_copy(
            src_ref=src, dst_ref=dst, send_sem=send, recv_sem=recv, device_id=(q, t), device_id_type=MESH
        )

    def update(w, m1, m2, g):
        whole = w[...] - LEARN_RATE * (HOLD_RATE * m1[...] + m2[...])
        w[...] = whole
        sums = jnp.sum(jnp.abs(whole), axis=0, keepdims=True)
        if g == 0:
            direct[f] = sums
        else:
            part[row] = sums

    def share(slots, slot, recv, to, send=None):
        for q in to:
            remote(slots.at[slot], slots.at[slot], sent.at[2] if send is None else send, recv, q).start()

    def wait_slots(slots, n, sem):
        pltpu.make_async_copy(slots.at[pl.ds(0, n)], slots.at[pl.ds(0, n)], sem).wait()

    def leave_early(i):
        r, n, s, _ = UNITS[0][EARLY[i]]
        for k, q in enumerate((at(s, 0, 0), at(-s, 0, 0), at(0, 1, 0))):
            remote(whole_g.at[pl.ds(r, n)], early.at[k, pl.ds(EARLY_AT[i], n)], sent.at[3], early_recv.at[0], q).start()

    def narrow(g, w):
        slots, n = (direct, 15) if g == 0 else (total, 3)
        wait_slots(slots, n, sums_recv.at[g])
        mean = jnp.sum(slots[...], axis=0) / d_model
        scale[g][...] = mean
        inverse = 1.0 / mean
        serve[g][f] = (w[...] * inverse).astype(jnp.bfloat16)
        return inverse

    def rows(g, u, block):
        return serve[g].at[block, pl.ds(UNITS[g][u][0], UNITS[g][u][1])]

    def send(g, u, kind, block, q):
        k = SEMAPHORES[g].index(semaphore_of(g, kind, u))
        remote(rows(g, u, block), rows(g, u, block), sent.at[g], tree_recv.at[g, k], q).start()

    def arrived(g, kind, u):
        key = semaphore_of(g, kind, u)
        ref = serve[g].at[0, pl.ds(0, TOGETHER[g][key])]
        pltpu.make_async_copy(ref, ref, tree_recv.at[g, SEMAPHORES[g].index(key)]).wait()

    def give(g, dy, dp, units=None):
        block = at(dy, dp, 0)
        for ref in [serve[g].at[block]] if units is None else [rows(g, u, block) for u in units]:
            remote(ref, ref, sent.at[g], d2d_recv.at[g], at(0, 0, 1)).start()

    def own(g):
        for u, (_, _, s, _) in enumerate(UNITS[g][:4]):
            send(g, u, "A", f, at(s, 0, 0))
            send(g, u, "C", f, at(0, 1, 0))
            send(g, u, "B", f, at(-s, 0, 0))

    for load in loads[:3]:
        load.wait()
    update(whole_g, a1, a2, 0)
    pl.semaphore_wait(barrier, len(peers) + z + side)
    share(direct, f, sums_recv.at[0], peers)
    for load in loads[3:]:
        load.wait()
    update(whole_u, b1, b2, 1)
    share(part, row, sums_recv.at[2], row_peers)

    own_norm[...] = jnp.zeros_like(own_norm)
    own_norm[0:1, 0:24] = (n0[...] + n1[...]).astype(jnp.bfloat16).astype(jnp.float32)
    first = 24 * t + 64 * (f % 2)
    rolled = pltpu.roll(jnp.broadcast_to(own_norm[0:1, :], (8, 128)), first % 128, 1)
    place = 128 * lax.broadcasted_iota(jnp.int32, (8, 128), 0) + lax.broadcasted_iota(jnp.int32, (8, 128), 1) - first
    near[row] = jnp.where((place >= 0) & (place < 24), rolled, 0.0)[0:2]
    share(near, row, norm_recv.at[0], row_peers, norm_sent.at[0])
    leave_early(0)
    leave_early(1)
    for q in tp_peers:

        @pl.when(t > q)
        def _(q=q):
            pl.semaphore_signal(here, inc=1, device_id=(f, q), device_id_type=MESH)

    wait_slots(part, 3, sums_recv.at[2])
    total[y] = jnp.sum(part[...], axis=0)
    share(total, y, sums_recv.at[1], ring_peers)
    wait_slots(near, 3, norm_recv.at[0])
    far[y] = near[...]
    share(far, y, norm_recv.at[1], ring_peers, norm_sent.at[1])

    inverse = narrow(0, whole_g)
    own(0)
    pltpu.make_async_copy(early, early, early_recv.at[0]).wait()
    for i, u in enumerate(EARLY):
        r, n, s, _ = UNITS[0][u]
        for k, q in enumerate((at(-s, 0, 0), at(s, 0, 0), at(0, 1, 0))):
            serve_g[q, r : r + n] = (early[k, EARLY_AT[i] : EARLY_AT[i] + n] * inverse).astype(jnp.bfloat16)
    for u in EARLY:
        s = UNITS[0][u][2]
        send(0, u, "D", at(-s, 0, 0), at(s, 0, 0))
        send(0, u, "E", at(-s, 0, 0), at(0, 1, 0))
        send(0, u, "F", at(0, 1, 0), at(-s, 0, 0))
    wait_slots(far, 3, norm_recv.at[1])
    norm[...] = jnp.zeros_like(norm)
    for i in range(16):
        r = 3 * i // 2
        norm[r : r + 2, :] = norm[r : r + 2, :] + far[i // 4, i % 4]
    image[0] = norm[0:24, :].astype(jnp.bfloat16)

    @pl.when(t < 7)
    def _():
        pl.semaphore_wait(here, 4 - z - side)

    def norm_to(src, dst, k, q):
        return pltpu.make_async_remote_copy(
            src_ref=src, dst_ref=dst, send_sem=norm_sent.at[k], recv_sem=norm_recv.at[k],
            device_id=(f, q), device_id_type=MESH,
        )

    norm_to(image.at[0], image.at[1], 2, tp_peers[3]).start()
    narrow(1, whole_u)
    own(1)
    for g in (0, 1):
        give(g, 0, 0)

    for g in (0, 1):
        for u, (_, _, s, crossings) in enumerate(UNITS[g][:4]):
            arrived(g, "A", u)
            send(g, u, "D", at(-s, 0, 0), at(s, 0, 0))
            send(g, u, "E", at(-s, 0, 0), at(0, 1, 0))
            if crossings == 2:
                arrived(g, "C", u)
                send(g, u, "F", at(0, 1, 0), at(-s, 0, 0))
        arrived(g, "C", 2)
        give(g, 0, 1)
    wait_slots(image, 1, norm_recv.at[2])
    stack[z] = (image[0].astype(jnp.float32) + image[1].astype(jnp.float32)).astype(jnp.bfloat16)
    for q in tp_peers[:3]:
        norm_to(stack.at[z], stack.at[z], 3, q).start()
    for g in (0, 1):
        for u in (2, 3):
            s = UNITS[g][u][2]
            arrived(g, "B", u)
            send(g, u, "F", at(s, 0, 0), at(0, 1, 0))
        arrived(g, "B", 0)
        give(g, 1, 0)
        give(g, 3, 0)

    for g in (0, 1):
        for u in (*EARLY, 0, 1, 2, 3) if g == 0 else range(4):
            s = UNITS[g][u][2]
            arrived(g, "E", u)
            send(g, u, "G", at(-s, 1, 0), at(s, 0, 0))
    for g in (0, 1):
        arrived(g, "D", 0)
        give(g, 2, 0)

    wait_slots(stack, 3, norm_recv.at[3])
    norm_out[...] = jnp.sum(stack[...].astype(jnp.float32), axis=0).astype(jnp.bfloat16)

    for g in (0, 1):
        arrived(g, "F", 0)
        both = (0, 1, *EARLY) if g == 0 else (0, 1)
        give(g, 1, 1, (*both, 3))
        give(g, 3, 1, (*both, 2))
    for g in (0, 1):
        arrived(g, "G", 0)
        give(g, 2, 1, (0, 1, *EARLY) if g == 0 else (0, 1))
        arrived(g, "F", 2)
        give(g, 1, 1, (2,))
        give(g, 3, 1, (3,))
        arrived(g, "G", 2)
        give(g, 2, 1, (2, 3))

    for g in (0, 1):
        pltpu.make_async_copy(serve[g].at[pl.ds(0, 8)], serve[g].at[pl.ds(0, 8)], d2d_recv.at[g]).wait()
    n = sum(unit[1] for unit in UNITS[0])
    blocks, rest = divmod(sum(TOGETHER[0].values()) + 8 * n, n)
    for ref, sem in (
        (serve_g.at[pl.ds(0, blocks)], sent.at[0]),
        (serve_g.at[0, pl.ds(0, rest)], sent.at[0]),
        (serve_u.at[pl.ds(0, 15)], sent.at[1]),
        (direct.at[pl.ds(0, 15)], sent.at[2]),
        (part.at[pl.ds(0, 3)], sent.at[2]),
        (total.at[pl.ds(0, 3)], sent.at[2]),
        (early, sent.at[3]),
        (near.at[pl.ds(0, 3)], norm_sent.at[0]),
        (far.at[pl.ds(0, 3)], norm_sent.at[1]),
        (image.at[0], norm_sent.at[2]),
        (stack.at[pl.ds(0, 3)], norm_sent.at[3]),
    ):
        pltpu.make_async_copy(ref, ref, sem).wait()


def keep(*refs):
    n = len(refs) // 2
    copies = [pltpu.make_async_copy(refs[i], refs[n + i], refs[-1].at[i]) for i in range(n)]
    for cp in copies:
        cp.start()
    for cp in copies:
        cp.wait()


def per_device(d_model, *args):
    rows, cols = args[0].shape
    f32, bf16 = jnp.float32, jnp.bfloat16
    any_space, vmem = pl.BlockSpec(memory_space=pl.ANY), pl.BlockSpec(memory_space=pltpu.VMEM)
    dma = pltpu.SemaphoreType.DMA
    shapes = (
        ((16, rows, cols), bf16),
        ((16, rows, cols), bf16),
        ((1, cols), f32),
        ((1, cols), f32),
        ((24, 128), bf16),
        ((rows, cols), f32),
        ((rows, cols), f32),
    )
    args = (*args[:6], *(a.reshape(1, -1) for a in args[6:]))
    args = [pltpu.with_memory_space_constraint(a, pltpu.HBM) for a in args]
    held = pl.pallas_call(
        functools.partial(kernel, d_model),
        name="step",
        out_shape=tuple(pltpu.VMEM(*shape) for shape in shapes),
        in_specs=[any_space] * 8,
        out_specs=[vmem] * 7,
        scratch_shapes=[
            *[pltpu.VMEM((rows, cols), f32)] * 4,
            *[pltpu.VMEM((1, 24), f32)] * 2,
            pltpu.VMEM((16, 1, cols), f32),
            pltpu.VMEM((4, 1, cols), f32),
            pltpu.VMEM((4, 1, cols), f32),
            pltpu.VMEM((8, 128), f32),
            pltpu.VMEM((4, 2, 128), f32),
            pltpu.VMEM((4, 4, 2, 128), f32),
            pltpu.VMEM((2, 24, 128), bf16),
            pltpu.VMEM((4, 24, 128), bf16),
            pltpu.VMEM((32, 128), f32),
            pltpu.VMEM((3, EARLY_ROWS, cols), f32),
            dma((8,)), dma((4,)), dma((2, max(map(len, SEMAPHORES)))), dma((3,)), dma((4,)), dma((4,)), dma((2,)), dma((1,)),
            pltpu.SemaphoreType.REGULAR,
        ],
        compiler_params=pltpu.CompilerParams(collective_id=0, has_side_effects=True, vmem_limit_bytes=16 * 2**20),
    )(*args)
    outs = pl.pallas_call(
        keep,
        name="keep",
        out_shape=tuple(jax.ShapeDtypeStruct(*shape) for shape in shapes),
        in_specs=[vmem] * 7,
        out_specs=[any_space] * 7,
        scratch_shapes=[dma((7,))],
        compiler_params=pltpu.CompilerParams(has_side_effects=True, vmem_limit_bytes=2**20),
    )(*[pltpu.with_memory_space_constraint(a, pltpu.VMEM) for a in held])
    serving_gate, serving_up, scale_gate, scale_up, norm, whole_gate, whole_up = outs
    return (
        serving_gate.reshape(16 * rows, cols),
        serving_up.reshape(16 * rows, cols),
        scale_gate.reshape(cols),
        scale_up.reshape(cols),
        norm.reshape(-1),
        whole_gate,
        whole_up,
    )


def solution(mesh):
    split = P("fsdp", "tp")
    return jax.shard_map(
        functools.partial(per_device, 3072),
        mesh=mesh,
        in_specs=(split,) * 6 + (P(("fsdp", "tp")),) * 2,
        out_specs=(P(None, "tp"), P(None, "tp"), P("tp"), P("tp"), P(), split, split),
        check_vma=False,
    )
```

```python
import functools

import jax
import jax.numpy as jnp
from jax import lax
from jax.experimental import pallas as pl
from jax.experimental.pallas import tpu as pltpu
from jax.sharding import PartitionSpec as P

MESH = pl.DeviceIdType.MESH
LEARN_RATE = 0.25
HOLD_RATE = 0.9

UNITS = (
    ((0, 40, 1, 2), (96, 40, -1, 2), (64, 32, 1, 3), (160, 32, -1, 3), (40, 24, 1, 2), (136, 24, -1, 2)),
    ((0, 64, 1, 2), (96, 64, -1, 2), (64, 32, 1, 3), (160, 32, -1, 3)),
)
EARLY = (4, 5)
EARLY_AT = (0, 24)
EARLY_ROWS = 48
KINDS = "ABCDEFG"


def semaphore_of(g, kind, u):
    three = UNITS[g][u][3] == 3
    if kind in "AE" or (kind == "C" and not three):
        return kind, u & 6 if u > 1 else u
    return kind, 9 if kind in "BFG" and three else 8


SEMAPHORES, TOGETHER = [], []
for matrix in (0, 1):
    rows_of = {}
    for kind in KINDS:
        for u, unit in enumerate(UNITS[matrix]):
            if matrix == 1 or u not in EARLY or kind not in "ABC":
                key = semaphore_of(matrix, kind, u)
                rows_of[key] = rows_of.get(key, 0) + unit[1]
    SEMAPHORES.append(sorted(rows_of))
    TOGETHER.append(rows_of)


def kernel(
    d_model, wg, fg, sg, wu, fu, su, nt, ns,
    serve_g, serve_u, scale_g, scale_u, norm_out, whole_g, whole_u,
    a1, a2, b1, b2, n0, n1, direct, part, total, own_norm, near, far, image, stack, norm, early,
    in_sem, sent, tree_recv, sums_recv, norm_recv, d2d_recv, early_recv, here,
):
    f, t = lax.axis_index("fsdp"), lax.axis_index("tp")
    y, p, c = f // 4, (f // 2) % 2, f % 2

    def at(dy, dp, dc):
        return ((y + dy + 4) % 4) * 4 + ((p + dp) % 2) * 2 + (c + dc) % 2

    peers = [at(dy, dp, dc) for dy in (2, 1, 3, 0) for dp in (1, 0) for dc in (1, 0) if (dy, dp, dc) != (0, 0, 0)]
    row, row_peers = f % 4, [at(0, 1, 1), at(0, 1, 0), at(0, 0, 1)]
    ring_peers = [at(2, 0, 0), at(1, 0, 0), at(3, 0, 0)]
    z, side = t // 2, t % 2
    tp_peers = [(t + 2 * k) % 8 for k in range(1, 4)] + [2 * z + 1 - side]

    barrier = pltpu.get_barrier_semaphore()
    for q in peers:
        pl.semaphore_signal(barrier, inc=1, device_id=(q, t), device_id_type=MESH)
    for q in tp_peers:

        @pl.when(t < q)
        def _(q=q):
            pl.semaphore_signal(barrier, inc=1, device_id=(f, q), device_id_type=MESH)

    serve, scale = (serve_g, serve_u), (scale_g, scale_u)
    pairs = ((wg, whole_g), (fg, a1), (sg, a2), (wu, whole_u), (fu, b1), (su, b2), (nt, n0), (ns, n1))
    loads = [pltpu.make_async_copy(src, dst, in_sem.at[i // 3]) for i, (src, dst) in enumerate(pairs)]
    for load in loads:
        load.start()

    def remote(src, dst, send, recv, q):
        return pltpu.make_async_remote_copy(
            src_ref=src, dst_ref=dst, send_sem=send, recv_sem=recv, device_id=(q, t), device_id_type=MESH
        )

    def update(w, m1, m2, g):
        whole = w[...] - LEARN_RATE * (HOLD_RATE * m1[...] + m2[...])
        w[...] = whole
        sums = jnp.sum(jnp.abs(whole), axis=0, keepdims=True)
        if g == 0:
            direct[f] = sums
        else:
            part[row] = sums

    def share(slots, slot, recv, to):
        for q in to:
            remote(slots.at[slot], slots.at[slot], sent.at[2], recv, q).start()

    def wait_slots(slots, n, sem):
        pltpu.make_async_copy(slots.at[pl.ds(0, n)], slots.at[pl.ds(0, n)], sem).wait()

    def leave_early(i):
        r, n, s, _ = UNITS[0][EARLY[i]]
        for k, q in enumerate((at(s, 0, 0), at(-s, 0, 0), at(0, 1, 0))):
            src, dst = whole_g.at[pl.ds(r, n)], early.at[k, pl.ds(EARLY_AT[i], n)]
            remote(src, dst, sent.at[3], early_recv.at[0], q).start()

    def narrow(g, w):
        slots, n = (direct, 15) if g == 0 else (total, 3)
        wait_slots(slots, n, sums_recv.at[g])
        mean = jnp.sum(slots[...], axis=0) / d_model
        scale[g][...] = mean
        inverse = 1.0 / mean
        serve[g][f] = (w[...] * inverse).astype(jnp.bfloat16)
        return inverse

    def rows(g, u, block):
        return serve[g].at[block, pl.ds(UNITS[g][u][0], UNITS[g][u][1])]

    def send(g, u, kind, block, q):
        k = SEMAPHORES[g].index(semaphore_of(g, kind, u))
        remote(rows(g, u, block), rows(g, u, block), sent.at[g], tree_recv.at[g, k], q).start()

    def arrived(g, kind, u):
        key = semaphore_of(g, kind, u)
        ref = serve[g].at[0, pl.ds(0, TOGETHER[g][key])]
        pltpu.make_async_copy(ref, ref, tree_recv.at[g, SEMAPHORES[g].index(key)]).wait()

    def give(g, dy, dp, units=None):
        block = at(dy, dp, 0)
        for ref in [serve[g].at[block]] if units is None else [rows(g, u, block) for u in units]:
            remote(ref, ref, sent.at[g], d2d_recv.at[g], at(0, 0, 1)).start()

    def own(g):
        for u, (_, _, s, _) in enumerate(UNITS[g][:4]):
            send(g, u, "A", f, at(s, 0, 0))
            send(g, u, "C", f, at(0, 1, 0))
            send(g, u, "B", f, at(-s, 0, 0))

    for load in loads[:3]:
        load.wait()
    update(whole_g, a1, a2, 0)
    for load in loads[3:]:
        load.wait()
    update(whole_u, b1, b2, 1)

    own_norm[...] = jnp.zeros_like(own_norm)
    own_norm[0:1, 0:24] = (n0[...] + n1[...]).astype(jnp.bfloat16).astype(jnp.float32)
    first = 24 * t + 64 * (f % 2)
    rolled = pltpu.roll(jnp.broadcast_to(own_norm[0:1, :], (8, 128)), first % 128, 1)
    place = 128 * lax.broadcasted_iota(jnp.int32, (8, 128), 0) + lax.broadcasted_iota(jnp.int32, (8, 128), 1) - first
    near[row] = jnp.where((place >= 0) & (place < 24), rolled, 0.0)[0:2]

    pl.semaphore_wait(barrier, len(peers) + z + side)
    share(direct, f, sums_recv.at[0], peers)
    share(part, row, sums_recv.at[2], row_peers)
    share(near, row, norm_recv.at[0], row_peers)
    leave_early(0)
    leave_early(1)
    for q in tp_peers:

        @pl.when(t > q)
        def _(q=q):
            pl.semaphore_signal(here, inc=1, device_id=(f, q), device_id_type=MESH)

    wait_slots(part, 3, sums_recv.at[2])
    total[y] = jnp.sum(part[...], axis=0)
    share(total, y, sums_recv.at[1], ring_peers)
    wait_slots(near, 3, norm_recv.at[0])
    far[y] = near[...]
    share(far, y, norm_recv.at[1], ring_peers)

    inverse = narrow(0, whole_g)
    own(0)
    pltpu.make_async_copy(early, early, early_recv.at[0]).wait()
    for i, u in enumerate(EARLY):
        r, n, s, _ = UNITS[0][u]
        for k, q in enumerate((at(-s, 0, 0), at(s, 0, 0), at(0, 1, 0))):
            serve_g[q, r : r + n] = (early[k, EARLY_AT[i] : EARLY_AT[i] + n] * inverse).astype(jnp.bfloat16)
    for u in EARLY:
        s = UNITS[0][u][2]
        send(0, u, "D", at(-s, 0, 0), at(s, 0, 0))
        send(0, u, "E", at(-s, 0, 0), at(0, 1, 0))
        send(0, u, "F", at(0, 1, 0), at(-s, 0, 0))
    wait_slots(far, 3, norm_recv.at[1])
    norm[...] = jnp.zeros_like(norm)
    for i in range(16):
        r = 3 * i // 2
        norm[r : r + 2, :] = norm[r : r + 2, :] + far[i // 4, i % 4]
    image[0] = norm[0:24, :].astype(jnp.bfloat16)

    @pl.when(t < 7)
    def _():
        pl.semaphore_wait(here, 4 - z - side)

    def norm_to(src, dst, k, q):
        return pltpu.make_async_remote_copy(
            src_ref=src, dst_ref=dst, send_sem=sent.at[2], recv_sem=norm_recv.at[k],
            device_id=(f, q), device_id_type=MESH,
        )

    norm_to(image.at[0], image.at[1], 2, tp_peers[3]).start()
    narrow(1, whole_u)
    own(1)
    for g in (0, 1):
        give(g, 0, 0)

    for g in (0, 1):
        for units in ((0,), (1,), (2, 3)):
            arrived(g, "A", units[0])
            for u in units:
                s = UNITS[g][u][2]
                send(g, u, "D", at(-s, 0, 0), at(s, 0, 0))
                send(g, u, "E", at(-s, 0, 0), at(0, 1, 0))
            if units[0] < 2:
                arrived(g, "C", u)
                send(g, u, "F", at(0, 1, 0), at(-s, 0, 0))
        arrived(g, "C", 2)
        give(g, 0, 1)
    wait_slots(image, 1, norm_recv.at[2])
    stack[z] = (image[0].astype(jnp.float32) + image[1].astype(jnp.float32)).astype(jnp.bfloat16)
    for q in tp_peers[:3]:
        norm_to(stack.at[z], stack.at[z], 3, q).start()
    for g in (0, 1):
        arrived(g, "B", 2)
        for u in (2, 3):
            s = UNITS[g][u][2]
            send(g, u, "F", at(s, 0, 0), at(0, 1, 0))
        arrived(g, "B", 0)
        give(g, 1, 0)
        give(g, 3, 0)

    for g in (0, 1):
        for units in (EARLY, (0,), (1,), (2, 3)) if g == 0 else ((0,), (1,), (2, 3)):
            arrived(g, "E", units[0])
            for u in units:
                s = UNITS[g][u][2]
                send(g, u, "G", at(-s, 1, 0), at(s, 0, 0))
    for g in (0, 1):
        arrived(g, "D", 0)
        give(g, 2, 0)

    wait_slots(stack, 3, norm_recv.at[3])
    norm_out[...] = jnp.sum(stack[...].astype(jnp.float32), axis=0).astype(jnp.bfloat16)

    for g in (0, 1):
        arrived(g, "F", 0)
        both = (0, 1, *EARLY) if g == 0 else (0, 1)
        give(g, 1, 1, (*both, 3))
        give(g, 3, 1, (*both, 2))
    for g in (0, 1):
        arrived(g, "G", 0)
        give(g, 2, 1, (0, 1, *EARLY) if g == 0 else (0, 1))
        arrived(g, "F", 2)
        give(g, 1, 1, (2,))
        give(g, 3, 1, (3,))
        arrived(g, "G", 2)
        give(g, 2, 1, (2, 3))

    for g in (0, 1):
        pltpu.make_async_copy(serve[g].at[pl.ds(0, 8)], serve[g].at[pl.ds(0, 8)], d2d_recv.at[g]).wait()
    n = sum(unit[1] for unit in UNITS[0])
    blocks, rest = divmod(sum(TOGETHER[0].values()) + 8 * n, n)
    for ref, sem in (
        (serve_g.at[pl.ds(0, blocks)], sent.at[0]),
        (serve_g.at[0, pl.ds(0, rest)], sent.at[0]),
        (serve_u.at[pl.ds(0, 15)], sent.at[1]),
        (direct.at[pl.ds(0, 15)], sent.at[2]),
        (part.at[pl.ds(0, 3)], sent.at[2]),
        (total.at[pl.ds(0, 3)], sent.at[2]),
        (early, sent.at[3]),
        (near.at[pl.ds(0, 3)], sent.at[2]),
        (far.at[pl.ds(0, 3)], sent.at[2]),
        (image.at[0], sent.at[2]),
        (stack.at[pl.ds(0, 3)], sent.at[2]),
    ):
        pltpu.make_async_copy(ref, ref, sem).wait()


def keep(*refs):
    n = len(refs) // 2
    copies = [pltpu.make_async_copy(refs[i], refs[n + i], refs[-1].at[i]) for i in range(n)]
    for cp in copies:
        cp.start()
    for cp in copies:
        cp.wait()


def per_device(d_model, *args):
    rows, cols = args[0].shape
    f32, bf16 = jnp.float32, jnp.bfloat16
    any_space, vmem = pl.BlockSpec(memory_space=pl.ANY), pl.BlockSpec(memory_space=pltpu.VMEM)
    dma = pltpu.SemaphoreType.DMA
    shapes = (
        ((16, rows, cols), bf16),
        ((16, rows, cols), bf16),
        ((1, cols), f32),
        ((1, cols), f32),
        ((24, 128), bf16),
        ((rows, cols), f32),
        ((rows, cols), f32),
    )
    args = (*args[:6], *(a.reshape(1, -1) for a in args[6:]))
    args = [pltpu.with_memory_space_constraint(a, pltpu.HBM) for a in args]
    held = pl.pallas_call(
        functools.partial(kernel, d_model),
        name="step",
        out_shape=tuple(pltpu.VMEM(*shape) for shape in shapes),
        in_specs=[any_space] * 8,
        out_specs=[vmem] * 7,
        scratch_shapes=[
            *[pltpu.VMEM((rows, cols), f32)] * 4,
            *[pltpu.VMEM((1, 24), f32)] * 2,
            pltpu.VMEM((16, 1, cols), f32),
            pltpu.VMEM((4, 1, cols), f32),
            pltpu.VMEM((4, 1, cols), f32),
            pltpu.VMEM((8, 128), f32),
            pltpu.VMEM((4, 2, 128), f32),
            pltpu.VMEM((4, 4, 2, 128), f32),
            pltpu.VMEM((2, 24, 128), bf16),
            pltpu.VMEM((4, 24, 128), bf16),
            pltpu.VMEM((32, 128), f32),
            pltpu.VMEM((3, EARLY_ROWS, cols), f32),
            dma((3,)), dma((4,)), dma((2, max(map(len, SEMAPHORES)))), dma((3,)), dma((4,)), dma((2,)), dma((1,)),
            pltpu.SemaphoreType.REGULAR,
        ],
        compiler_params=pltpu.CompilerParams(collective_id=0, has_side_effects=True, vmem_limit_bytes=16 * 2**20),
    )(*args)
    outs = pl.pallas_call(
        keep,
        name="keep",
        out_shape=tuple(jax.ShapeDtypeStruct(*shape) for shape in shapes),
        in_specs=[vmem] * 7,
        out_specs=[any_space] * 7,
        scratch_shapes=[dma((7,))],
        compiler_params=pltpu.CompilerParams(has_side_effects=True, vmem_limit_bytes=2**20),
    )(*[pltpu.with_memory_space_constraint(a, pltpu.VMEM) for a in held])
    serving_gate, serving_up, scale_gate, scale_up, norm, whole_gate, whole_up = outs
    return (
        serving_gate.reshape(16 * rows, cols),
        serving_up.reshape(16 * rows, cols),
        scale_gate.reshape(cols),
        scale_up.reshape(cols),
        norm.reshape(-1),
        whole_gate,
        whole_up,
    )


def solution(mesh):
    split = P("fsdp", "tp")
    return jax.shard_map(
        functools.partial(per_device, 3072),
        mesh=mesh,
        in_specs=(split,) * 6 + (P(("fsdp", "tp")),) * 2,
        out_specs=(P(None, "tp"), P(None, "tp"), P("tp"), P("tp"), P(), split, split),
        check_vma=False,
    )
```

```python
import functools

import jax
import jax.numpy as jnp
from jax import lax
from jax.experimental import pallas as pl
from jax.experimental.pallas import tpu as pltpu
from jax.sharding import PartitionSpec as P

MESH = pl.DeviceIdType.MESH
LEARN_RATE = 0.25
HOLD_RATE = 0.9

UNITS = (
    ((0, 40, 1, 2), (96, 40, -1, 2), (64, 32, 1, 3), (160, 32, -1, 3), (40, 24, 1, 2), (136, 24, -1, 2)),
    ((0, 64, 1, 2), (96, 64, -1, 2), (64, 32, 1, 3), (160, 32, -1, 3)),
)
EARLY = (4, 5)
EARLY_AT = (0, 24)
EARLY_ROWS = 48
KINDS = "ABCDEFG"


def semaphore_of(g, kind, u):
    three = UNITS[g][u][3] == 3
    if kind in "AE" or (kind == "C" and not three):
        return kind, u & 6 if u > 1 else u
    if kind == "F" and three:
        return kind, u
    return kind, 9 if kind in "BG" and three else 8


SEMAPHORES, TOGETHER = [], []
for matrix in (0, 1):
    rows_of = {}
    for kind in KINDS:
        for u, unit in enumerate(UNITS[matrix]):
            if matrix == 1 or u not in EARLY or kind not in "ABC":
                key = semaphore_of(matrix, kind, u)
                rows_of[key] = rows_of.get(key, 0) + unit[1]
    SEMAPHORES.append(sorted(rows_of))
    TOGETHER.append(rows_of)


def kernel(
    d_model, wg, fg, sg, wu, fu, su, nt, ns,
    serve_g, serve_u, scale_g, scale_u, norm_out, whole_g, whole_u,
    a1, a2, b1, b2, n0, n1, direct, part, total, own_norm, near, far, image, stack, norm, early,
    in_sem, sent, tree_recv, sums_recv, norm_recv, d2d_recv, early_recv, here,
):
    f, t = lax.axis_index("fsdp"), lax.axis_index("tp")
    y, p, c = f // 4, (f // 2) % 2, f % 2

    def at(dy, dp, dc):
        return ((y + dy + 4) % 4) * 4 + ((p + dp) % 2) * 2 + (c + dc) % 2

    peers = [at(dy, dp, dc) for dy in (2, 1, 3, 0) for dp in (1, 0) for dc in (1, 0) if (dy, dp, dc) != (0, 0, 0)]
    row, row_peers = f % 4, [at(0, 1, 1), at(0, 1, 0), at(0, 0, 1)]
    ring_peers = [at(2, 0, 0), at(1, 0, 0), at(3, 0, 0)]
    z, side = t // 2, t % 2
    tp_peers = [(t + 2 * k) % 8 for k in range(1, 4)] + [2 * z + 1 - side]

    barrier = pltpu.get_barrier_semaphore()
    for q in peers:
        pl.semaphore_signal(barrier, inc=1, device_id=(q, t), device_id_type=MESH)
    for q in tp_peers:

        @pl.when(t < q)
        def _(q=q):
            pl.semaphore_signal(barrier, inc=1, device_id=(f, q), device_id_type=MESH)

    serve, scale = (serve_g, serve_u), (scale_g, scale_u)
    pairs = ((wg, whole_g), (fg, a1), (sg, a2), (wu, whole_u), (fu, b1), (su, b2), (nt, n0), (ns, n1))
    loads = [pltpu.make_async_copy(src, dst, in_sem.at[i // 3]) for i, (src, dst) in enumerate(pairs)]
    for load in loads:
        load.start()

    def remote(src, dst, send, recv, q):
        return pltpu.make_async_remote_copy(
            src_ref=src, dst_ref=dst, send_sem=send, recv_sem=recv, device_id=(q, t), device_id_type=MESH
        )

    def update(w, m1, m2, g):
        whole = w[...] - LEARN_RATE * (HOLD_RATE * m1[...] + m2[...])
        w[...] = whole
        sums = jnp.sum(jnp.abs(whole), axis=0, keepdims=True)
        if g == 0:
            direct[f] = sums
        else:
            part[row] = sums

    def share(slots, slot, recv, to):
        for q in to:
            remote(slots.at[slot], slots.at[slot], sent.at[2], recv, q).start()

    def wait_slots(slots, n, sem):
        pltpu.make_async_copy(slots.at[pl.ds(0, n)], slots.at[pl.ds(0, n)], sem).wait()

    def leave_early(i):
        r, n, s, _ = UNITS[0][EARLY[i]]
        for k, q in enumerate((at(s, 0, 0), at(-s, 0, 0), at(0, 1, 0))):
            src, dst = whole_g.at[pl.ds(r, n)], early.at[k, pl.ds(EARLY_AT[i], n)]
            remote(src, dst, sent.at[3], early_recv.at[0], q).start()

    def narrow(g, w):
        slots, n = (direct, 15) if g == 0 else (total, 3)
        wait_slots(slots, n, sums_recv.at[g])
        mean = jnp.sum(slots[...], axis=0) / d_model
        scale[g][...] = mean
        inverse = 1.0 / mean
        serve[g][f] = (w[...] * inverse).astype(jnp.bfloat16)
        return inverse

    def rows(g, u, block):
        return serve[g].at[block, pl.ds(UNITS[g][u][0], UNITS[g][u][1])]

    def send(g, u, kind, block, q):
        k = SEMAPHORES[g].index(semaphore_of(g, kind, u))
        remote(rows(g, u, block), rows(g, u, block), sent.at[g], tree_recv.at[g, k], q).start()

    def arrived(g, kind, u):
        key = semaphore_of(g, kind, u)
        ref = serve[g].at[0, pl.ds(0, TOGETHER[g][key])]
        pltpu.make_async_copy(ref, ref, tree_recv.at[g, SEMAPHORES[g].index(key)]).wait()

    def give(g, dy, dp, units=None):
        block = at(dy, dp, 0)
        for ref in [serve[g].at[block]] if units is None else [rows(g, u, block) for u in units]:
            remote(ref, ref, sent.at[g], d2d_recv.at[g], at(0, 0, 1)).start()

    def own(g):
        for u, (_, _, s, _) in enumerate(UNITS[g][:4]):
            send(g, u, "A", f, at(s, 0, 0))
            send(g, u, "C", f, at(0, 1, 0))
            send(g, u, "B", f, at(-s, 0, 0))

    for load in loads[:3]:
        load.wait()
    update(whole_g, a1, a2, 0)
    for load in loads[3:]:
        load.wait()
    update(whole_u, b1, b2, 1)

    own_norm[...] = jnp.zeros_like(own_norm)
    own_norm[0:1, 0:24] = (n0[...] + n1[...]).astype(jnp.bfloat16).astype(jnp.float32)
    first = 24 * t + 64 * (f % 2)
    rolled = pltpu.roll(jnp.broadcast_to(own_norm[0:1, :], (8, 128)), first % 128, 1)
    place = 128 * lax.broadcasted_iota(jnp.int32, (8, 128), 0) + lax.broadcasted_iota(jnp.int32, (8, 128), 1) - first
    near[row] = jnp.where((place >= 0) & (place < 24), rolled, 0.0)[0:2]

    pl.semaphore_wait(barrier, len(peers) + z + side)
    share(direct, f, sums_recv.at[0], peers)
    share(part, row, sums_recv.at[2], row_peers)
    share(near, row, norm_recv.at[0], row_peers)
    leave_early(0)
    leave_early(1)
    for q in tp_peers:

        @pl.when(t > q)
        def _(q=q):
            pl.semaphore_signal(here, inc=1, device_id=(f, q), device_id_type=MESH)

    wait_slots(part, 3, sums_recv.at[2])
    total[y] = jnp.sum(part[...], axis=0)
    share(total, y, sums_recv.at[1], ring_peers)
    wait_slots(near, 3, norm_recv.at[0])
    far[y] = near[...]
    share(far, y, norm_recv.at[1], ring_peers)

    inverse = narrow(0, whole_g)
    own(0)
    pltpu.make_async_copy(early, early, early_recv.at[0]).wait()
    for i, u in enumerate(EARLY):
        r, n, s, _ = UNITS[0][u]
        for k, q in enumerate((at(-s, 0, 0), at(s, 0, 0), at(0, 1, 0))):
            serve_g[q, r : r + n] = (early[k, EARLY_AT[i] : EARLY_AT[i] + n] * inverse).astype(jnp.bfloat16)
    for u in EARLY:
        s = UNITS[0][u][2]
        send(0, u, "D", at(-s, 0, 0), at(s, 0, 0))
        send(0, u, "E", at(-s, 0, 0), at(0, 1, 0))
        send(0, u, "F", at(0, 1, 0), at(-s, 0, 0))
    wait_slots(far, 3, norm_recv.at[1])
    norm[...] = jnp.zeros_like(norm)
    for i in range(16):
        r = 3 * i // 2
        norm[r : r + 2, :] = norm[r : r + 2, :] + far[i // 4, i % 4]
    image[0] = norm[0:24, :].astype(jnp.bfloat16)

    @pl.when(t < 7)
    def _():
        pl.semaphore_wait(here, 4 - z - side)

    def norm_to(src, dst, k, q):
        return pltpu.make_async_remote_copy(
            src_ref=src, dst_ref=dst, send_sem=sent.at[2], recv_sem=norm_recv.at[k],
            device_id=(f, q), device_id_type=MESH,
        )

    norm_to(image.at[0], image.at[1], 2, tp_peers[3]).start()
    narrow(1, whole_u)
    own(1)
    for g in (0, 1):
        give(g, 0, 0)

    for g in (0, 1):
        for units in ((0,), (1,), (2, 3)):
            arrived(g, "A", units[0])
            for u in units:
                s = UNITS[g][u][2]
                send(g, u, "D", at(-s, 0, 0), at(s, 0, 0))
                send(g, u, "E", at(-s, 0, 0), at(0, 1, 0))
            if units[0] < 2:
                arrived(g, "C", u)
                send(g, u, "F", at(0, 1, 0), at(-s, 0, 0))
        arrived(g, "C", 2)
        give(g, 0, 1)
    wait_slots(image, 1, norm_recv.at[2])
    stack[z] = (image[0].astype(jnp.float32) + image[1].astype(jnp.float32)).astype(jnp.bfloat16)
    for q in tp_peers[:3]:
        norm_to(stack.at[z], stack.at[z], 3, q).start()
    for g in (0, 1):
        arrived(g, "B", 2)
        for u in (2, 3):
            s = UNITS[g][u][2]
            send(g, u, "F", at(s, 0, 0), at(0, 1, 0))
        arrived(g, "B", 0)
        give(g, 1, 0)
        give(g, 3, 0)

    for g in (0, 1):
        for units in (EARLY, (0,), (1,), (2, 3)) if g == 0 else ((0,), (1,), (2, 3)):
            arrived(g, "E", units[0])
            for u in units:
                s = UNITS[g][u][2]
                send(g, u, "G", at(-s, 1, 0), at(s, 0, 0))
    for g in (0, 1):
        arrived(g, "D", 0)
        give(g, 2, 0)

    wait_slots(stack, 3, norm_recv.at[3])
    norm_out[...] = jnp.sum(stack[...].astype(jnp.float32), axis=0).astype(jnp.bfloat16)

    for g in (0, 1):
        arrived(g, "F", 0)
        both = (0, 1, *EARLY) if g == 0 else (0, 1)
        give(g, 1, 1, (*both, 3))
        give(g, 3, 1, (*both, 2))
    for g in (0, 1):
        arrived(g, "G", 0)
        give(g, 2, 1, (0, 1, *EARLY) if g == 0 else (0, 1))
        arrived(g, "F", 2)
        give(g, 1, 1, (2,))
        arrived(g, "G", 2)
        give(g, 2, 1, (2, 3))
        arrived(g, "F", 3)
        give(g, 3, 1, (3,))

    for g in (0, 1):
        pltpu.make_async_copy(serve[g].at[pl.ds(0, 8)], serve[g].at[pl.ds(0, 8)], d2d_recv.at[g]).wait()
    n = sum(unit[1] for unit in UNITS[0])
    blocks, rest = divmod(sum(TOGETHER[0].values()) + 8 * n, n)
    for ref, sem in (
        (serve_g.at[pl.ds(0, blocks)], sent.at[0]),
        (serve_g.at[0, pl.ds(0, rest)], sent.at[0]),
        (serve_u.at[pl.ds(0, 15)], sent.at[1]),
        (direct.at[pl.ds(0, 15)], sent.at[2]),
        (part.at[pl.ds(0, 3)], sent.at[2]),
        (total.at[pl.ds(0, 3)], sent.at[2]),
        (early, sent.at[3]),
        (near.at[pl.ds(0, 3)], sent.at[2]),
        (far.at[pl.ds(0, 3)], sent.at[2]),
        (image.at[0], sent.at[2]),
        (stack.at[pl.ds(0, 3)], sent.at[2]),
    ):
        pltpu.make_async_copy(ref, ref, sem).wait()


def keep(*refs):
    n = len(refs) // 2
    copies = [pltpu.make_async_copy(refs[i], refs[n + i], refs[-1].at[i]) for i in range(n)]
    for cp in copies:
        cp.start()
    for cp in copies:
        cp.wait()


def per_device(d_model, *args):
    rows, cols = args[0].shape
    f32, bf16 = jnp.float32, jnp.bfloat16
    any_space, vmem = pl.BlockSpec(memory_space=pl.ANY), pl.BlockSpec(memory_space=pltpu.VMEM)
    dma = pltpu.SemaphoreType.DMA
    shapes = (
        ((16, rows, cols), bf16),
        ((16, rows, cols), bf16),
        ((1, cols), f32),
        ((1, cols), f32),
        ((24, 128), bf16),
        ((rows, cols), f32),
        ((rows, cols), f32),
    )
    args = (*args[:6], *(a.reshape(1, -1) for a in args[6:]))
    args = [pltpu.with_memory_space_constraint(a, pltpu.HBM) for a in args]
    held = pl.pallas_call(
        functools.partial(kernel, d_model),
        name="step",
        out_shape=tuple(pltpu.VMEM(*shape) for shape in shapes),
        in_specs=[any_space] * 8,
        out_specs=[vmem] * 7,
        scratch_shapes=[
            *[pltpu.VMEM((rows, cols), f32)] * 4,
            *[pltpu.VMEM((1, 24), f32)] * 2,
            pltpu.VMEM((16, 1, cols), f32),
            pltpu.VMEM((4, 1, cols), f32),
            pltpu.VMEM((4, 1, cols), f32),
            pltpu.VMEM((8, 128), f32),
            pltpu.VMEM((4, 2, 128), f32),
            pltpu.VMEM((4, 4, 2, 128), f32),
            pltpu.VMEM((2, 24, 128), bf16),
            pltpu.VMEM((4, 24, 128), bf16),
            pltpu.VMEM((32, 128), f32),
            pltpu.VMEM((3, EARLY_ROWS, cols), f32),
            dma((3,)), dma((4,)), dma((2, max(map(len, SEMAPHORES)))), dma((3,)), dma((4,)), dma((2,)), dma((1,)),
            pltpu.SemaphoreType.REGULAR,
        ],
        compiler_params=pltpu.CompilerParams(collective_id=0, has_side_effects=True, vmem_limit_bytes=16 * 2**20),
    )(*args)
    outs = pl.pallas_call(
        keep,
        name="keep",
        out_shape=tuple(jax.ShapeDtypeStruct(*shape) for shape in shapes),
        in_specs=[vmem] * 7,
        out_specs=[any_space] * 7,
        scratch_shapes=[dma((7,))],
        compiler_params=pltpu.CompilerParams(has_side_effects=True, vmem_limit_bytes=2**20),
    )(*[pltpu.with_memory_space_constraint(a, pltpu.VMEM) for a in held])
    serving_gate, serving_up, scale_gate, scale_up, norm, whole_gate, whole_up = outs
    return (
        serving_gate.reshape(16 * rows, cols),
        serving_up.reshape(16 * rows, cols),
        scale_gate.reshape(cols),
        scale_up.reshape(cols),
        norm.reshape(-1),
        whole_gate,
        whole_up,
    )


def solution(mesh):
    split = P("fsdp", "tp")
    return jax.shard_map(
        functools.partial(per_device, 3072),
        mesh=mesh,
        in_specs=(split,) * 6 + (P(("fsdp", "tp")),) * 2,
        out_specs=(P(None, "tp"), P(None, "tp"), P("tp"), P("tp"), P(), split, split),
        check_vma=False,
    )
```

```python
import functools

import jax
import jax.numpy as jnp
from jax import lax
from jax.experimental import pallas as pl
from jax.experimental.pallas import tpu as pltpu
from jax.sharding import PartitionSpec as P

MESH = pl.DeviceIdType.MESH
LEARN_RATE = 0.25
HOLD_RATE = 0.9

UNITS = (
    ((0, 40, 1, 2), (96, 40, -1, 2), (64, 32, 1, 3), (160, 32, -1, 3), (40, 24, 1, 2), (136, 24, -1, 2)),
    ((0, 64, 1, 2), (96, 64, -1, 2), (64, 32, 1, 3), (160, 32, -1, 3)),
)
EARLY = (4, 5)
EARLY_AT = (0, 24)
EARLY_ROWS = 48
KINDS = "ABCDEFG"


def semaphore_of(g, kind, u):
    three = UNITS[g][u][3] == 3
    if kind in "AE" or (kind == "C" and not three):
        return kind, u & 6 if u > 1 else u
    if kind == "F" and three:
        return kind, u
    return kind, 9 if kind == "G" and three else 8


SEMAPHORES, TOGETHER = [], []
for matrix in (0, 1):
    rows_of = {}
    for kind in KINDS:
        for u, unit in enumerate(UNITS[matrix]):
            if matrix == 1 or u not in EARLY or kind not in "ABC":
                key = semaphore_of(matrix, kind, u)
                rows_of[key] = rows_of.get(key, 0) + unit[1]
    SEMAPHORES.append(sorted(rows_of))
    TOGETHER.append(rows_of)


def kernel(
    d_model, wg, fg, sg, wu, fu, su, nt, ns,
    serve_g, serve_u, scale_g, scale_u, norm_out, whole_g, whole_u,
    a1, a2, b1, b2, n0, n1, direct, part, total, own_norm, near, far, image, stack, norm, early,
    in_sem, sent, tree_recv, sums_recv, norm_recv, d2d_recv, early_recv, here,
):
    f, t = lax.axis_index("fsdp"), lax.axis_index("tp")
    y, p, c = f // 4, (f // 2) % 2, f % 2

    def at(dy, dp, dc):
        return ((y + dy + 4) % 4) * 4 + ((p + dp) % 2) * 2 + (c + dc) % 2

    peers = [at(dy, dp, dc) for dy in (2, 1, 3, 0) for dp in (1, 0) for dc in (1, 0) if (dy, dp, dc) != (0, 0, 0)]
    row, row_peers = f % 4, [at(0, 1, 1), at(0, 1, 0), at(0, 0, 1)]
    ring_peers = [at(2, 0, 0), at(1, 0, 0), at(3, 0, 0)]
    z, side = t // 2, t % 2
    tp_peers = [(t + 2 * k) % 8 for k in range(1, 4)] + [2 * z + 1 - side]

    barrier = pltpu.get_barrier_semaphore()
    for q in peers:
        pl.semaphore_signal(barrier, inc=1, device_id=(q, t), device_id_type=MESH)
    for q in tp_peers:

        @pl.when(t < q)
        def _(q=q):
            pl.semaphore_signal(barrier, inc=1, device_id=(f, q), device_id_type=MESH)

    serve, scale = (serve_g, serve_u), (scale_g, scale_u)
    pairs = ((wg, whole_g), (fg, a1), (sg, a2), (wu, whole_u), (fu, b1), (su, b2), (nt, n0), (ns, n1))
    loads = [pltpu.make_async_copy(src, dst, in_sem.at[i // 3]) for i, (src, dst) in enumerate(pairs)]
    for load in loads:
        load.start()

    def remote(src, dst, send, recv, q):
        return pltpu.make_async_remote_copy(
            src_ref=src, dst_ref=dst, send_sem=send, recv_sem=recv, device_id=(q, t), device_id_type=MESH
        )

    def update(w, m1, m2, g):
        whole = w[...] - LEARN_RATE * (HOLD_RATE * m1[...] + m2[...])
        w[...] = whole
        sums = jnp.sum(jnp.abs(whole), axis=0, keepdims=True)
        if g == 0:
            direct[f] = sums
        else:
            part[row] = sums

    def share(slots, slot, recv, to):
        for q in to:
            remote(slots.at[slot], slots.at[slot], sent.at[2], recv, q).start()

    def wait_slots(slots, n, sem):
        pltpu.make_async_copy(slots.at[pl.ds(0, n)], slots.at[pl.ds(0, n)], sem).wait()

    def leave_early(i):
        r, n, s, _ = UNITS[0][EARLY[i]]
        for k, q in enumerate((at(s, 0, 0), at(-s, 0, 0), at(0, 1, 0))):
            src, dst = whole_g.at[pl.ds(r, n)], early.at[k, pl.ds(EARLY_AT[i], n)]
            remote(src, dst, sent.at[3], early_recv.at[0], q).start()

    def narrow(g, w):
        slots, n = (direct, 15) if g == 0 else (total, 3)
        wait_slots(slots, n, sums_recv.at[g])
        mean = jnp.sum(slots[...], axis=0) / d_model
        scale[g][...] = mean
        inverse = 1.0 / mean
        serve[g][f] = (w[...] * inverse).astype(jnp.bfloat16)
        return inverse

    def rows(g, u, block):
        return serve[g].at[block, pl.ds(UNITS[g][u][0], UNITS[g][u][1])]

    def send(g, u, kind, block, q):
        k = SEMAPHORES[g].index(semaphore_of(g, kind, u))
        remote(rows(g, u, block), rows(g, u, block), sent.at[g], tree_recv.at[g, k], q).start()

    def arrived(g, kind, u):
        key = semaphore_of(g, kind, u)
        ref = serve[g].at[0, pl.ds(0, TOGETHER[g][key])]
        pltpu.make_async_copy(ref, ref, tree_recv.at[g, SEMAPHORES[g].index(key)]).wait()

    def give(g, dy, dp, units=None):
        block = at(dy, dp, 0)
        for ref in [serve[g].at[block]] if units is None else [rows(g, u, block) for u in units]:
            remote(ref, ref, sent.at[g], d2d_recv.at[g], at(0, 0, 1)).start()

    def own(g):
        for u, (_, _, s, _) in enumerate(UNITS[g][:4]):
            send(g, u, "A", f, at(s, 0, 0))
            send(g, u, "C", f, at(0, 1, 0))
            send(g, u, "B", f, at(-s, 0, 0))

    for load in loads[:3]:
        load.wait()
    update(whole_g, a1, a2, 0)
    for load in loads[3:]:
        load.wait()
    update(whole_u, b1, b2, 1)

    own_norm[...] = jnp.zeros_like(own_norm)
    own_norm[0:1, 0:24] = (n0[...] + n1[...]).astype(jnp.bfloat16).astype(jnp.float32)
    first = 24 * t + 64 * (f % 2)
    rolled = pltpu.roll(jnp.broadcast_to(own_norm[0:1, :], (8, 128)), first % 128, 1)
    place = 128 * lax.broadcasted_iota(jnp.int32, (8, 128), 0) + lax.broadcasted_iota(jnp.int32, (8, 128), 1) - first
    near[row] = jnp.where((place >= 0) & (place < 24), rolled, 0.0)[0:2]

    pl.semaphore_wait(barrier, len(peers) + z + side)
    share(direct, f, sums_recv.at[0], peers)
    share(part, row, sums_recv.at[2], row_peers)
    share(near, row, norm_recv.at[0], row_peers)
    leave_early(0)
    leave_early(1)
    for q in tp_peers:

        @pl.when(t > q)
        def _(q=q):
            pl.semaphore_signal(here, inc=1, device_id=(f, q), device_id_type=MESH)

    wait_slots(part, 3, sums_recv.at[2])
    total[y] = jnp.sum(part[...], axis=0)
    share(total, y, sums_recv.at[1], ring_peers)
    wait_slots(near, 3, norm_recv.at[0])
    far[y] = near[...]
    share(far, y, norm_recv.at[1], ring_peers)

    inverse = narrow(0, whole_g)
    own(0)
    pltpu.make_async_copy(early, early, early_recv.at[0]).wait()
    for i, u in enumerate(EARLY):
        r, n, s, _ = UNITS[0][u]
        for k, q in enumerate((at(-s, 0, 0), at(s, 0, 0), at(0, 1, 0))):
            serve_g[q, r : r + n] = (early[k, EARLY_AT[i] : EARLY_AT[i] + n] * inverse).astype(jnp.bfloat16)
    for u in EARLY:
        s = UNITS[0][u][2]
        send(0, u, "D", at(-s, 0, 0), at(s, 0, 0))
        send(0, u, "E", at(-s, 0, 0), at(0, 1, 0))
        send(0, u, "F", at(0, 1, 0), at(-s, 0, 0))
    wait_slots(far, 3, norm_recv.at[1])
    norm[...] = jnp.zeros_like(norm)
    for i in range(16):
        r = 3 * i // 2
        norm[r : r + 2, :] = norm[r : r + 2, :] + far[i // 4, i % 4]
    image[0] = norm[0:24, :].astype(jnp.bfloat16)

    @pl.when(t < 7)
    def _():
        pl.semaphore_wait(here, 4 - z - side)

    def norm_to(src, dst, k, q):
        return pltpu.make_async_remote_copy(
            src_ref=src, dst_ref=dst, send_sem=sent.at[2], recv_sem=norm_recv.at[k],
            device_id=(f, q), device_id_type=MESH,
        )

    norm_to(image.at[0], image.at[1], 2, tp_peers[3]).start()
    narrow(1, whole_u)
    own(1)
    for g in (0, 1):
        give(g, 0, 0)

    for g in (0, 1):
        for units in ((0,), (1,), (2, 3)):
            arrived(g, "A", units[0])
            for u in units:
                s = UNITS[g][u][2]
                send(g, u, "D", at(-s, 0, 0), at(s, 0, 0))
                send(g, u, "E", at(-s, 0, 0), at(0, 1, 0))
            if units[0] < 2:
                arrived(g, "C", u)
                send(g, u, "F", at(0, 1, 0), at(-s, 0, 0))
        arrived(g, "C", 2)
        give(g, 0, 1)
    wait_slots(image, 1, norm_recv.at[2])
    stack[z] = (image[0].astype(jnp.float32) + image[1].astype(jnp.float32)).astype(jnp.bfloat16)
    for q in tp_peers[:3]:
        norm_to(stack.at[z], stack.at[z], 3, q).start()
    for g in (0, 1):
        arrived(g, "B", 2)
        for u in (2, 3):
            s = UNITS[g][u][2]
            send(g, u, "F", at(s, 0, 0), at(0, 1, 0))
        give(g, 1, 0)
        give(g, 3, 0)

    for g in (0, 1):
        for units in (EARLY, (0,), (1,), (2, 3)) if g == 0 else ((0,), (1,), (2, 3)):
            arrived(g, "E", units[0])
            for u in units:
                s = UNITS[g][u][2]
                send(g, u, "G", at(-s, 1, 0), at(s, 0, 0))
    for g in (0, 1):
        arrived(g, "D", 0)
        give(g, 2, 0)

    wait_slots(stack, 3, norm_recv.at[3])
    norm_out[...] = jnp.sum(stack[...].astype(jnp.float32), axis=0).astype(jnp.bfloat16)

    for g in (0, 1):
        arrived(g, "F", 0)
        both = (0, 1, *EARLY) if g == 0 else (0, 1)
        give(g, 1, 1, (*both, 3))
        give(g, 3, 1, (*both, 2))
    for g in (0, 1):
        arrived(g, "G", 0)
        give(g, 2, 1, (0, 1, *EARLY) if g == 0 else (0, 1))
        arrived(g, "F", 2)
        give(g, 1, 1, (2,))
        arrived(g, "G", 2)
        give(g, 2, 1, (2, 3))
        arrived(g, "F", 3)
        give(g, 3, 1, (3,))

    for g in (0, 1):
        pltpu.make_async_copy(serve[g].at[pl.ds(0, 8)], serve[g].at[pl.ds(0, 8)], d2d_recv.at[g]).wait()
    n = sum(unit[1] for unit in UNITS[0])
    blocks, rest = divmod(sum(TOGETHER[0].values()) + 8 * n, n)
    for ref, sem in (
        (serve_g.at[pl.ds(0, blocks)], sent.at[0]),
        (serve_g.at[0, pl.ds(0, rest)], sent.at[0]),
        (serve_u.at[pl.ds(0, 15)], sent.at[1]),
        (direct.at[pl.ds(0, 15)], sent.at[2]),
        (part.at[pl.ds(0, 3)], sent.at[2]),
        (total.at[pl.ds(0, 3)], sent.at[2]),
        (early, sent.at[3]),
        (near.at[pl.ds(0, 3)], sent.at[2]),
        (far.at[pl.ds(0, 3)], sent.at[2]),
        (image.at[0], sent.at[2]),
        (stack.at[pl.ds(0, 3)], sent.at[2]),
    ):
        pltpu.make_async_copy(ref, ref, sem).wait()


def keep(*refs):
    n = len(refs) // 2
    copies = [pltpu.make_async_copy(refs[i], refs[n + i], refs[-1]) for i in range(n)]
    for cp in copies:
        cp.start()
    for cp in copies:
        cp.wait()


def per_device(d_model, *args):
    rows, cols = args[0].shape
    f32, bf16 = jnp.float32, jnp.bfloat16
    any_space, vmem = pl.BlockSpec(memory_space=pl.ANY), pl.BlockSpec(memory_space=pltpu.VMEM)
    dma = pltpu.SemaphoreType.DMA
    shapes = (
        ((16, rows, cols), bf16),
        ((16, rows, cols), bf16),
        ((1, cols), f32),
        ((1, cols), f32),
        ((24, 128), bf16),
        ((rows, cols), f32),
        ((rows, cols), f32),
    )
    args = (*args[:6], *(a.reshape(1, -1) for a in args[6:]))
    args = [pltpu.with_memory_space_constraint(a, pltpu.HBM) for a in args]
    held = pl.pallas_call(
        functools.partial(kernel, d_model),
        name="step",
        out_shape=tuple(pltpu.VMEM(*shape) for shape in shapes),
        in_specs=[any_space] * 8,
        out_specs=[vmem] * 7,
        scratch_shapes=[
            *[pltpu.VMEM((rows, cols), f32)] * 4,
            *[pltpu.VMEM((1, 24), f32)] * 2,
            pltpu.VMEM((16, 1, cols), f32),
            pltpu.VMEM((4, 1, cols), f32),
            pltpu.VMEM((4, 1, cols), f32),
            pltpu.VMEM((8, 128), f32),
            pltpu.VMEM((4, 2, 128), f32),
            pltpu.VMEM((4, 4, 2, 128), f32),
            pltpu.VMEM((2, 24, 128), bf16),
            pltpu.VMEM((4, 24, 128), bf16),
            pltpu.VMEM((32, 128), f32),
            pltpu.VMEM((3, EARLY_ROWS, cols), f32),
            dma((3,)), dma((4,)), dma((2, max(map(len, SEMAPHORES)))), dma((3,)), dma((4,)), dma((2,)), dma((1,)),
            pltpu.SemaphoreType.REGULAR,
        ],
        compiler_params=pltpu.CompilerParams(collective_id=0, has_side_effects=True, vmem_limit_bytes=16 * 2**20),
    )(*args)
    outs = pl.pallas_call(
        keep,
        name="keep",
        out_shape=tuple(jax.ShapeDtypeStruct(*shape) for shape in shapes),
        in_specs=[vmem] * 7,
        out_specs=[any_space] * 7,
        scratch_shapes=[dma],
        compiler_params=pltpu.CompilerParams(has_side_effects=True, vmem_limit_bytes=2**20),
    )(*[pltpu.with_memory_space_constraint(a, pltpu.VMEM) for a in held])
    serving_gate, serving_up, scale_gate, scale_up, norm, whole_gate, whole_up = outs
    return (
        serving_gate.reshape(16 * rows, cols),
        serving_up.reshape(16 * rows, cols),
        scale_gate.reshape(cols),
        scale_up.reshape(cols),
        norm.reshape(-1),
        whole_gate,
        whole_up,
    )


def solution(mesh):
    split = P("fsdp", "tp")
    return jax.shard_map(
        functools.partial(per_device, 3072),
        mesh=mesh,
        in_specs=(split,) * 6 + (P(("fsdp", "tp")),) * 2,
        out_specs=(P(None, "tp"), P(None, "tp"), P("tp"), P("tp"), P(), split, split),
        check_vma=False,
    )
```
